256 devices in a mesh: rep: 2 (over z), exp: 8 (over x), ten: 16 (over y, core).
Axes of the slice: x: 8, y: 8, z: 2, core: 2. Of those that a mesh axis runs over, the one named last changes fastest.
The devices are a block of a 8x8x16 slice.
Arguments:
- hidden_in: bfloat16 [6144, 3072], P(('rep', 'exp', 'ten')), parts along dimension 0, may hold values from -6 to 6
- queries: bfloat16 [6144, 6144], P(('rep', 'exp', 'ten')), parts along dimension 0, may hold values from -100 to 100
- new_kv: bfloat16 [2, 6144, 1024], P(None, ('rep', 'exp', 'ten')), parts along dimension 1, may hold values from -5 to 5
- prefix_kv: bfloat16 [2, 16, 512, 1024], P(None, ('rep', 'exp'), 'ten'), parts along dimension 1, may hold values from -5 to 5
- decode_kv: bfloat16 [2, 1024, 48, 1024], P(None, ('rep', 'exp', 'ten')), parts along dimension 1, may hold values from -5 to 5
- prefix_len: int32 [16], P(('rep', 'exp')), parts along dimension 0, may hold values from 2 to 512
- decode_len: int32 [1024], P(('rep', 'exp', 'ten')), parts along dimension 0, may hold values from 2 to 48
- out_proj: bfloat16 [6144, 3072], P('ten'), may hold values from -0.078125 to 0.078125
- norm_gain: float32 [3072], replicated, may hold values from 0.5 to 1.5
- router_w: bfloat16 [3072, 8], replicated, may hold values from -0.109375 to 0.109375
- expert_ids: int32 [6144, 2], P(('rep', 'exp', 'ten')), parts along dimension 0, may hold values from 0 to 7, all different within a row; in each aligned block of 24 rows (0 to 23, 24 to 47, ...) at most 7 rows name the same one
- w_gate: bfloat16 [8, 3072, 8192], P('exp', None, 'ten'), may hold values from -0.109375 to 0.109375
- w_up: bfloat16 [8, 3072, 8192], P('exp', None, 'ten'), may hold values from -0.109375 to 0.109375
- w_down: bfloat16 [8, 8192, 3072], P('exp', 'ten'), may hold values from -0.0625 to 0.0625
Outputs:
- layer_out: bfloat16 [6144, 3072], P(('rep', 'exp', 'ten')), parts along dimension 0
The draws below stay inside these ranges and needn't reach their ends.
There are 2 independent parts, one for each index of `rep`. The reference program is written for one: setup_inputs(seed, part) draws one part's arguments, and reference() takes and returns one part's arrays. A program takes and returns all parts, laid end to end along the dimension named above; an argument that names none is the same for every part. Nothing has to cross between parts.
Inputs may be any that keep to these rules, and one draw needn't show every extreme that they name: `expert_ids`: each row names two different experts. Within each aligned block of 24 rows (the rows of one device) no expert is named by more than 7 rows, and in some block one expert is named by exactly 7 rows.
All inputs are finite; a program needn't handle non-finite values.
Results may differ from the reference program's by a relative error of at most 0.013.
Values may be sent and summed in bfloat16 or wider, within the bound.
A program may use at most 128 MiB of HBM per device.

```python
import math
import jax
import jax.numpy as jnp
import numpy as np
from jax import lax

D = 3072
FF = 8192
HQ = 48
KVH = 8
HD = 128
EXPERTS = 8
ROWS_DEV = 24
DEC_DEV = 4
CTX_DEC = 48
CAP = 7
CH_DEV = 20
GROUP_ROWS = 384
SPAN = 320
DEC_GROUP = 64
TOKENS = 3072
PREFIX = 512
DEC_ALL = 512
N_EXP = 8
N_TEN = 16


def joint_fields(key):
    base_key = jax.random.fold_in(key, 4417)
    key_query, key_prefix, key_decode = jax.random.split(base_key, 3)
    query_field = jnp.clip(jax.random.normal(key_query, (N_EXP, GROUP_ROWS, HQ, HD), jnp.float32), -5.0, 5.0)
    prefix_field = jnp.clip(jax.random.normal(key_prefix, (2, N_EXP, PREFIX, KVH, HD), jnp.float32), -5.0, 5.0)
    decode_field = jnp.clip(jax.random.normal(key_decode, (2, DEC_ALL, CTX_DEC, KVH, HD), jnp.float32), -5.0, 5.0)
    return (query_field, prefix_field, decode_field)


def draw_queries(key, part):
    return joint_fields(key)[0].reshape(TOKENS, HQ * HD).astype(jnp.bfloat16)


def draw_prefix_kv(key, part):
    return joint_fields(key)[1].reshape(2, N_EXP, PREFIX, KVH * HD).astype(jnp.bfloat16)


def draw_decode_kv(key, part):
    return joint_fields(key)[2].reshape(2, DEC_ALL, CTX_DEC, KVH * HD).astype(jnp.bfloat16)


def plant(entries, key, smallest, high):
    spot = [jax.random.randint(jax.random.fold_in(key, axis), (), 0, length) for axis, length in enumerate(entries.shape)]
    main_axis = entries.shape.index(max(entries.shape))
    neighbour = spot[:main_axis] + [(spot[main_axis] + 1) % entries.shape[main_axis]] + spot[main_axis + 1:]
    return entries.at[tuple(spot)].set(smallest).at[tuple(neighbour)].set(high)


def block_scale(stream_key, dims, cuts, smallest, top_value):
    factor_of = 1.0
    for position, blocks in cuts:
        steps = jax.random.uniform(jax.random.fold_in(jax.random.fold_in(stream_key, 6), position), (blocks,), jnp.float32, smallest / len(cuts), top_value / len(cuts))
        factor_of = factor_of * jnp.repeat(jnp.exp(steps), dims[position] // blocks).reshape((-1,) + (1,) * (len(dims) - 1 - position))
    return factor_of


def deal_out(key, own, number, rows, number_of, top, reach, skew):
    sequence = jax.random.permutation(key, number_of)
    packed, usual = load_shares(number_of, rows * top, reach, skew, True), load_shares(number_of, rows * top, reach, skew, False)
    places = jnp.arange(number_of)

    def named(sizes, offset_by):
        used = int((sizes > 0).sum())
        fixed = max(1, used // 4)
        shifted = fixed + (places - fixed + offset_by * (used - fixed)) % max(1, number_of - fixed)
        return jnp.zeros((number_of,), jnp.int32).at[sequence[jnp.where(places < fixed, places, shifted)]].set(jnp.asarray(sizes, jnp.int32))

    sizes = jnp.where(number % 4 == 0, named(packed, number // 4), named(usual, number - number // 4 - 1))
    mixed = jax.random.permutation(jax.random.fold_in(own, 3), number_of)
    giver, receiver = mixed[0:number_of // 2 * 2:2], mixed[1:number_of // 2 * 2:2]
    slack = jnp.minimum(sizes[giver] - 1, reach - sizes[receiver]) // 2
    slack = jnp.where((giver == sequence[0]) | (receiver == sequence[0]) | (sizes[receiver] == 0), 0, jnp.maximum(slack, 0))
    shifted = jax.random.randint(jax.random.fold_in(own, 4), (number_of // 2,), 0, 1 << 20) % (slack + 1)
    sizes = sizes.at[giver].add(-shifted).at[receiver].add(shifted)
    items = jnp.searchsorted(jnp.cumsum(sizes), jnp.arange(rows * top), side="right").astype(jnp.int32)
    grid = items.reshape(top, rows).T
    grid = grid[jax.random.permutation(jax.random.fold_in(own, 1), rows)]
    offset_by = jax.random.randint(jax.random.fold_in(own, 2), (rows, 1), 0, top)
    return jnp.take_along_axis(grid, (jnp.arange(top)[None, :] + offset_by) % top, axis=1)


def load_shares(number_of, total, reach, slope, full):
    portions = [(1 << 20) // math.isqrt(grade ** slope) + 1 for grade in range(1, number_of + 1)]
    largest = reach if full else min(reach, max(-(-total // number_of), total * portions[0] // sum(portions)))
    least = 1 if total - largest >= number_of - 1 else 0
    given, surplus = [largest] + [least] * (number_of - 1), total - largest - least * (number_of - 1)
    while surplus > 0:
        free = [i for i in range(1, number_of) if given[i] < largest] or [i for i in range(1, number_of) if given[i] < reach]
        whole, left = sum([portions[i] for i in free]), surplus
        for i in free:
            more = min(reach - given[i], max(1, left * portions[i] // whole), surplus)
            given[i] = given[i] + more
            surplus = surplus - more
    return np.array(given)


def noise(stream_key, shape, deviation, bound, shards=(), kind=jnp.bfloat16):
    loudness = block_scale(stream_key, shape, shards, -0.22, 0.18) if shards else 1.0
    entries = jax.random.normal(stream_key, shape, jnp.float32) * deviation * loudness
    return jnp.minimum(jnp.maximum(entries, -bound), bound).astype(kind)


def setup_inputs(seed: int = 0, part: int = 0) -> dict:
    splits = jax.random.split(jax.random.key(seed), 15)
    part_keys = jax.random.split(jax.random.fold_in(splits[14], part), 15)
    hidden_in = noise(part_keys[0], (TOKENS, D), 1.0, 6.0, ((0, 128),))
    queries = draw_queries(jax.random.fold_in(jax.random.fold_in(splits[14], part), 71), part)
    new_kv = noise(part_keys[2], (2, TOKENS, KVH * HD), 1.0, 5.0, ((1, 128),))
    prefix_kv = draw_prefix_kv(jax.random.fold_in(jax.random.fold_in(splits[14], part), 71), part)
    decode_kv = draw_decode_kv(jax.random.fold_in(jax.random.fold_in(splits[14], part), 71), part)
    prefix_len = plant(jax.random.randint(part_keys[5], (N_EXP,), 2, PREFIX + 1), jax.random.fold_in(part_keys[5], 1), 2, PREFIX).astype(jnp.int32)
    decode_len = plant(jax.random.randint(part_keys[6], (DEC_ALL,), 2, CTX_DEC + 1), jax.random.fold_in(part_keys[6], 1), 2, CTX_DEC).astype(jnp.int32)
    out_proj = noise(splits[7], (HQ * HD, D), (HQ * HD) ** -0.5, 0.078125, ((0, 16),))
    norm_gain = jnp.clip(1.0 + 0.1 * jax.random.normal(splits[8], (D,), jnp.float32), 0.5, 1.5)
    router_w = noise(splits[9], (D, EXPERTS), D ** -0.5, 0.109375)
    expert_ids_keys = jax.random.split(jax.random.fold_in(part_keys[10], 1), TOKENS // ROWS_DEV)
    expert_ids_turns = jax.random.permutation(jax.random.fold_in(part_keys[10], 3), TOKENS // ROWS_DEV)
    expert_ids = jax.vmap(lambda own, number: deal_out(jax.random.fold_in(part_keys[10], 2), own, number, ROWS_DEV, EXPERTS, 2, CAP, 2))(expert_ids_keys, expert_ids_turns).reshape((TOKENS, 2))
    w_gate = noise(splits[11], (EXPERTS, D, FF), D ** -0.5, 0.109375, ((0, 8), (2, 16)))
    w_up = noise(splits[12], (EXPERTS, D, FF), D ** -0.5, 0.109375, ((0, 8), (2, 16)))
    w_down = noise(splits[13], (EXPERTS, FF, D), FF ** -0.5, 0.0625, ((0, 8), (1, 16)))
    return {"hidden_in": hidden_in, "queries": queries, "new_kv": new_kv, "prefix_kv": prefix_kv, "decode_kv": decode_kv, "prefix_len": prefix_len, "decode_len": decode_len, "out_proj": out_proj, "norm_gain": norm_gain, "router_w": router_w, "expert_ids": expert_ids, "w_gate": w_gate, "w_up": w_up, "w_down": w_down}


def attend(scores, visible, values, pattern):
    masked = jnp.where(visible, scores, -jnp.inf)
    row_max = lax.optimization_barrier(jnp.max(masked, axis=-1, keepdims=True))
    exponent = jnp.exp(masked - row_max)
    totals = lax.optimization_barrier(jnp.sum(exponent, axis=-1))
    weights = exponent.astype(jnp.bfloat16).astype(jnp.float32)
    return (jnp.einsum(pattern, weights, values) / totals[..., None]).astype(jnp.bfloat16)

def group_attention(group, queries, new_kv, prefix_kv, decode_kv, prefix_len, decode_len):
    per_kv = HQ // KVH
    score_scale = HD ** (-0.5)
    first_row = group * GROUP_ROWS
    query_rows = queries[first_row:first_row + GROUP_ROWS].astype(jnp.float32).reshape(N_TEN, ROWS_DEV, KVH, per_kv, HD)
    key_rows = new_kv[0, first_row:first_row + GROUP_ROWS].astype(jnp.float32).reshape(N_TEN, ROWS_DEV, KVH, HD)
    value_rows = new_kv[1, first_row:first_row + GROUP_ROWS].astype(jnp.float32).reshape(N_TEN, ROWS_DEV, KVH, HD)
    span_queries = query_rows[:, :CH_DEV].reshape(SPAN, KVH, per_kv, HD)
    span_keys = key_rows[:, :CH_DEV].reshape(SPAN, KVH, HD)
    span_values = value_rows[:, :CH_DEV].reshape(SPAN, KVH, HD)
    prefill_keys = jnp.concatenate([prefix_kv[0, group].astype(jnp.float32).reshape(PREFIX, KVH, HD), span_keys], axis=0)
    prefill_values = jnp.concatenate([prefix_kv[1, group].astype(jnp.float32).reshape(PREFIX, KVH, HD), span_values], axis=0)
    scores = jnp.einsum('rcgh,pch->rcgp', span_queries, prefill_keys) * score_scale
    positions = jnp.arange(PREFIX + SPAN, dtype=jnp.int32)[None, :]
    row_index = jnp.arange(SPAN, dtype=jnp.int32)[:, None]
    visible = jnp.where(positions < PREFIX, positions < prefix_len[group], positions - PREFIX <= row_index)
    prefill_out = attend(scores, visible[:, None, None, :], prefill_values, 'rcgp,pch->rcgh')
    first_seq = group * DEC_GROUP
    dec_queries = query_rows[:, CH_DEV:].reshape(DEC_GROUP, KVH, per_kv, HD)
    own_keys = key_rows[:, CH_DEV:].reshape(DEC_GROUP, KVH, HD)
    own_values = value_rows[:, CH_DEV:].reshape(DEC_GROUP, KVH, HD)
    decode_keys = jnp.concatenate([decode_kv[0, first_seq:first_seq + DEC_GROUP].astype(jnp.float32).reshape(DEC_GROUP, CTX_DEC, KVH, HD), own_keys[:, None]], axis=1)
    decode_values = jnp.concatenate([decode_kv[1, first_seq:first_seq + DEC_GROUP].astype(jnp.float32).reshape(DEC_GROUP, CTX_DEC, KVH, HD), own_values[:, None]], axis=1)
    decode_scores = jnp.einsum('dcgh,dpch->dcgp', dec_queries, decode_keys) * score_scale
    decode_pos = jnp.arange(CTX_DEC + 1, dtype=jnp.int32)[None, :]
    lengths = decode_len[first_seq:first_seq + DEC_GROUP][:, None]
    visible_dec = (decode_pos < lengths) | (decode_pos == CTX_DEC)
    decode_out = attend(decode_scores, visible_dec[:, None, None, :], decode_values, 'dcgp,dpch->dcgh')
    combined = jnp.concatenate([prefill_out.reshape(N_TEN, CH_DEV, HQ * HD), decode_out.reshape(N_TEN, DEC_DEV, HQ * HD)], axis=1)
    return combined.reshape(GROUP_ROWS, HQ * HD)

def run_expert(bundle):
    slot_rows, gate_weight, up_weight, down_weight = bundle
    gate_act = jnp.dot(slot_rows, gate_weight, preferred_element_type=jnp.float32)
    up_act = jnp.dot(slot_rows, up_weight, preferred_element_type=jnp.float32)
    hidden = (jax.nn.silu(gate_act) * up_act).astype(jnp.bfloat16)
    return jnp.dot(hidden, down_weight, preferred_element_type=jnp.float32).astype(jnp.bfloat16)

def reference(hidden_in, queries, new_kv, prefix_kv, decode_kv, prefix_len, decode_len, out_proj, norm_gain, router_w, expert_ids, w_gate, w_up, w_down):
    pieces = []
    for group in range(N_EXP):
        pieces.append(group_attention(group, queries, new_kv, prefix_kv, decode_kv, prefix_len, decode_len))
    attended = jnp.concatenate(pieces, axis=0)
    residual = hidden_in.astype(jnp.float32) + jnp.dot(attended, out_proj, preferred_element_type=jnp.float32)
    mean_square = lax.optimization_barrier(jnp.mean(residual * residual, axis=1, keepdims=True))
    normed = (residual * lax.rsqrt(mean_square + 1e-05) * norm_gain).astype(jnp.bfloat16)
    logits = jnp.dot(normed, router_w, preferred_element_type=jnp.float32)
    chosen_logits = jnp.take_along_axis(logits, expert_ids, axis=1)
    route_weights = jax.nn.softmax(chosen_logits, axis=1)
    blocks = TOKENS // ROWS_DEV
    chosen = expert_ids.reshape(blocks, ROWS_DEV * 2)
    chosen_hot = (chosen[:, :, None] == jnp.arange(EXPERTS, dtype=jnp.int32)).astype(jnp.int32)
    earlier = jnp.cumsum(chosen_hot, axis=1) - chosen_hot
    slot_rank = lax.optimization_barrier(jnp.sum(earlier * chosen_hot, axis=2))
    slot_flat = (jnp.arange(blocks, dtype=jnp.int32)[:, None] * CAP + slot_rank).reshape(-1).astype(jnp.int32)
    expert_flat = expert_ids.reshape(-1).astype(jnp.int32)
    token_of = jnp.repeat(jnp.arange(TOKENS, dtype=jnp.int32), 2)
    buffer = jnp.zeros((EXPERTS, blocks * CAP, D), jnp.bfloat16).at[expert_flat, slot_flat].set(normed[token_of])
    expert_out = lax.map(run_expert, (buffer, w_gate, w_up, w_down))
    picked = expert_out[expert_flat, slot_flat].reshape(TOKENS, 2, D).astype(jnp.float32)
    mixed = residual + route_weights[:, 0:1] * picked[:, 0] + route_weights[:, 1:2] * picked[:, 1]
    return mixed.astype(jnp.bfloat16)
```

```python
import jax
import jax.numpy as jnp
from jax import lax
from jax.experimental import pallas as pl
from jax.experimental.pallas import tpu as pltpu
from jax.sharding import Mesh
from jax.sharding import PartitionSpec as P

MESH = pl.DeviceIdType.MESH
HD = 128
CAP = 7
F32 = jnp.float32
BF16 = jnp.bfloat16
NEG = -1e30
EXP, CHIP, CORE = "exp", "ten_0", "ten_1"
TEN = (CHIP, CORE)
REP_EXP_TEN = ("rep", EXP, CHIP, CORE)


def iota(shape, dim):
    return lax.broadcasted_iota(jnp.int32, shape, dim)


def cols(start, size):
    return pl.ds(pl.multiple_of(start, 128), size)


def rows(start, size, align):
    return pl.ds(pl.multiple_of(start, align), size)


def dot(a, b):
    return jnp.dot(a, b, preferred_element_type=F32)


def dot_t(a, b):
    return lax.dot_general(a, b, (((1,), (1,)), ((), ())), preferred_element_type=F32)


def ring_order(chips):
    far = chips // 2
    order = []
    for hop in range(far - 1, 0, -1):
        order += [(False, hop), (True, hop + 1)]
    return order + [(True, 1)]


class Copies:
    def __init__(self):
        self.sent = []

    def start(self, copy):
        copy.start()
        self.sent.append(copy)
        return copy

    def drain(self):
        for copy in self.sent:
            copy.wait_send()
        self.sent = []


def remote(src, dst, send_sem, recv_sem, **device):
    return pltpu.make_async_remote_copy(
        src_ref=src, dst_ref=dst, send_sem=send_sem, recv_sem=recv_sem,
        device_id=device, device_id_type=MESH,
    )


def ring_reduce(y, chips, copies, part, rs_out, rs_in, s_sem, r_sem, subs):
    order = ring_order(chips)
    place = {m: i for i, m in enumerate(order)}

    def copy(way, index, sub):
        to = lax.rem(y + (1 if way == 0 else chips - 1), chips)
        return remote(
            rs_out.at[way, index, sub], rs_in.at[way, index, sub],
            s_sem.at[way, index, sub], r_sem.at[way, index, sub], **{CHIP: to},
        )

    for index, (is_long, hop) in enumerate(order):
        for sub in range(subs):
            for way in range(2):
                half = (0 if is_long else 1) ^ way
                dest = lax.rem(y + (hop if way == 0 else chips - hop), chips)
                value = part(dest, half, sub)
                if (is_long, hop + 1) in place:
                    before = place[is_long, hop + 1]
                    copy(way, before, sub).wait_recv()
                    value = value + rs_in[way, before, sub].astype(F32)
                rs_out[way, index, sub] = value.astype(BF16)
                copies.start(copy(way, index, sub))

    def total(half, sub):
        value = part(y, half, sub)
        for way in range(2):
            last = place[(half ^ way) == 0, 1]
            copy(way, last, sub).wait_recv()
            value = value + rs_in[way, last, sub].astype(F32)
        return value

    return total


def k1_scratch(d):
    r, c, n = d["rows"], d["chips"], 2 * d["chips"]
    jw = d["heads_dev"] * HD
    half = d["model"] // 2
    msgs = len(ring_order(c))
    v, dma = pltpu.VMEM, pltpu.SemaphoreType.DMA
    return dict(
        q_v=v((r, d["heads_q"] * HD), BF16),
        nkv_v=v((2, r, d["kvw"]), BF16),
        pre_v=v((2, d["pre_dev"], d["kvw"]), BF16),
        dec_v=v((2, d["dec"], d["ctx"], d["kvw"]), BF16),
        qb=v((n, r, jw), BF16),
        kvn=v((2, c, 2, r, HD), BF16),
        kvp=v((2, c, 2, d["pre_dev"], HD), BF16),
        dec_o=v((d["heads_q"] * 8, HD), BF16),
        decs=v((n, 16, HD), BF16),
        decr=v((n, 16, HD), BF16),
        qh=v((d["heads_dev"] * n * r, HD), BF16),
        kall=v((n * (d["pre_dev"] + r), HD), BF16),
        vall=v((n * (d["pre_dev"] + r), HD), BF16),
        att=v((2, n * r, jw), BF16),
        wo=v((2, jw, half), BF16),
        part=v((n * r, half), F32),
        rs_out=v((2, msgs, 1, 2 * r, half // 2), BF16),
        rs_in=v((2, msgs, 1, 2 * r, half // 2), BF16),
        l_sem=dma((9,)),
        qs_sem=dma((n,)),
        qr_sem=dma((n,)),
        kns_sem=dma((c,)),
        knr_sem=dma((c,)),
        kps_sem=dma((c,)),
        kpr_sem=dma((c,)),
        x_s=dma((8,)),
        x_r=dma((8,)),
        ds_sem=dma((n,)),
        dr_sem=dma((n,)),
        rs_s=dma((2, msgs, 1)),
        rs_r=dma((2, msgs, 1)),
    )


def attend_and_project(d, S, y, k, copies, q_hbm, nkv_hbm, pre_hbm, dec_hbm, plen, dlen, wo_hbm, barrier):
    r, c, n, dec, span = d["rows"], d["chips"], 2 * d["chips"], d["dec"], d["rows"] - d["dec"]
    hq, per_kv, hd_dev, ctx, pre_dev = d["heads_q"], d["per_kv"], d["heads_dev"], d["ctx"], d["pre_dev"]
    jw, half = hd_dev * HD, d["model"] // 2
    t = 2 * y + k
    other = 1 - k
    scale = HD ** -0.5
    l_sem = S["l_sem"]

    def local(src, dst, i):
        copy = pltpu.make_async_copy(src, dst, l_sem.at[i])
        copy.start()
        return copy

    kv_cols = cols(y * HD, HD)
    l_n = local(nkv_hbm, S["nkv_v"], 0)
    l_p = local(pre_hbm.at[:, 0], S["pre_v"], 1)
    l_q = local(q_hbm, S["q_v"], 2)
    l_own = [
        local(nkv_hbm.at[:, :, kv_cols], S["kvn"].at[k, y], 3),
        local(pre_hbm.at[:, 0, :, kv_cols], S["kvp"].at[k, y], 4),
        local(q_hbm.at[:, cols(t * jw, jw)], S["qb"].at[t], 5),
    ]
    l_d = local(dec_hbm, S["dec_v"], 6)
    l_w = local(wo_hbm.at[:, cols(k * half, half)], S["wo"].at[k], 7)

    barrier()

    def kn_copy(src_y, to):
        return remote(
            S["nkv_v"].at[:, :, cols(to * HD, HD)], S["kvn"].at[k, src_y],
            S["kns_sem"].at[to], S["knr_sem"].at[src_y], **{CHIP: to},
        )

    def kp_copy(src_y, to):
        return remote(
            S["pre_v"].at[:, :, cols(to * HD, HD)], S["kvp"].at[k, src_y],
            S["kps_sem"].at[to], S["kpr_sem"].at[src_y], **{CHIP: to},
        )

    def q_copy(src_t, to_t):
        return remote(
            S["q_v"].at[:, cols(to_t * jw, jw)], S["qb"].at[src_t],
            S["qs_sem"].at[to_t], S["qr_sem"].at[src_t], **{CHIP: to_t // 2, CORE: to_t % 2},
        )

    l_n.wait()
    l_p.wait()
    for o in range(1, c):
        to = lax.rem(y + ((o + 1) // 2 if o % 2 else c - o // 2), c)
        copies.start(kn_copy(y, to))
        copies.start(kp_copy(y, to))
    l_q.wait()
    for o in range(c):
        to = y if o == 0 else lax.rem(y + ((o + 1) // 2 if o % 2 else c - o // 2), c)
        for kk in ([1] if o == 0 else [0, 1]):
            to_k = lax.rem(k + kk, 2)
            copies.start(q_copy(t, 2 * to + to_k))
    wo_copy = copies.start(remote(
        wo_hbm.at[:, cols(other * half, half)], S["wo"].at[k], S["x_s"].at[0], S["x_r"].at[0],
        **{CORE: other},
    ))

    l_d.wait()
    q8 = S["q_v"][16:24, :].astype(F32)
    n8 = [S["nkv_v"][i, 16:24, :].astype(F32) for i in range(2)]
    m = per_kv * 8
    keys = dec * ctx
    lane = iota((m, keys), 1)
    row8 = iota((m, keys), 0) & 7
    req = sum((lane >= ctx * i).astype(jnp.int32) for i in range(1, dec))
    pos = lane - ctx * req
    length = dlen[0]
    for i in range(1, dec):
        length = jnp.where(req == i, dlen[i], length)
    seen = (row8 - (8 - dec) == req) & (pos < length)
    for g in range(hq // per_kv):
        qg = jnp.concatenate(
            [q8[:, (g * per_kv + h) * HD : (g * per_kv + h + 1) * HD] for h in range(per_kv)], axis=0
        )
        kg = S["dec_v"][0, :, :, g * HD : (g + 1) * HD].reshape(keys, HD)
        vg = S["dec_v"][1, :, :, g * HD : (g + 1) * HD].reshape(keys, HD)
        own_k = jnp.concatenate([n8[0][:, g * HD : (g + 1) * HD]] * per_kv, axis=0)
        own_v = jnp.concatenate([n8[1][:, g * HD : (g + 1) * HD]] * per_kv, axis=0)
        s = jnp.where(seen, dot_t(qg.astype(BF16), kg) * scale, NEG)
        s_own = jnp.sum(qg * own_k, axis=1, keepdims=True) * scale
        top = jnp.maximum(jnp.max(s, axis=1, keepdims=True), s_own)
        p = jnp.where(seen, jnp.exp(s - top), 0.0)
        p_own = jnp.exp(s_own - top)
        den = jnp.sum(p, axis=1, keepdims=True) + p_own
        o = dot(p.astype(BF16), vg) + p_own.astype(BF16).astype(F32) * own_v
        S["dec_o"][g * m : (g + 1) * m, :] = (o / den).astype(BF16)
    to_row = iota((n * 16, hq * 8), 0)
    from_row = iota((n * 16, hq * 8), 1)
    slot = to_row & 15
    wanted = (to_row >> 4) * (8 * hd_dev) + (slot >> 2) * 8 + (8 - dec) + (slot & 3)
    pick = ((from_row == wanted) & (slot < hd_dev * dec)).astype(BF16)
    S["decs"][...] = dot(pick, S["dec_o"][...]).astype(BF16).reshape(n, 16, HD)

    def d_copy(src_t, to_t):
        return remote(
            S["decs"].at[to_t], S["decr"].at[src_t],
            S["ds_sem"].at[to_t], S["dr_sem"].at[src_t], **{CHIP: to_t // 2, CORE: to_t % 2},
        )

    for o in range(1, n):
        copies.start(d_copy(t, lax.rem(t + o, n)))
    S["decr"][t] = S["decs"][t]

    for copy in l_own:
        copy.wait()
    for o in range(1, c):
        src = lax.rem(y + o, c)
        kn_copy(src, y).wait_recv()
        kp_copy(src, y).wait_recv()
    relay = [
        copies.start(remote(S[b].at[k], S[b].at[k], S["x_s"].at[i], S["x_r"].at[i], **{CORE: other}))
        for i, b in ((1, "kvn"), (2, "kvp"))
    ]
    for o in range(1, n):
        q_copy(lax.rem(t + o, n), t).wait_recv()
    for cc in range(c):
        pair = [S["qb"][2 * cc + i].astype(F32) for i in range(2)]
        for j in range(hd_dev):
            S["qh"][j * n * r + cc * 2 * r : j * n * r + (cc + 1) * 2 * r, :] = jnp.concatenate(
                [q[:, j * HD : (j + 1) * HD] for q in pair], axis=0
            ).astype(BF16)
    for copy in relay:
        copy.wait_recv()
    prefix = n * pre_dev
    for i, b in ((0, "kall"), (1, "vall")):
        for cc in range(c):
            for kk in range(2):
                at = (2 * cc + kk) * pre_dev
                S[b][at : at + pre_dev, :] = S["kvp"][kk, cc, i]
            S[b][prefix + cc * 2 * r : prefix + (cc + 1) * 2 * r, :] = jnp.concatenate(
                [S["kvn"][kk, cc, i].astype(F32) for kk in range(2)], axis=0
            ).astype(BF16)
    for o in range(1, n):
        d_copy(lax.rem(t + o, n), t).wait_recv()

    block_devs = 4
    block = block_devs * r
    col = iota((1, n * r), 1)
    col_dev = sum((col >= r * i).astype(jnp.int32) for i in range(1, n))
    col_in = col - r * col_dev
    key_place = jnp.where(col_in < span, col_dev * span + col_in, 1 << 20)
    pre_seen = iota((1, prefix), 1) < plen[0]
    row = iota((block, 1), 0)
    row_dev = sum((row >= r * i).astype(jnp.int32) for i in range(1, block_devs))
    row_in = row - r * row_dev
    from_col = iota((block, n * 16), 1)

    def attend(b, carry):
        device = b * block_devs + row_dev
        place = device * span + row_in
        new_seen = key_place <= place
        first = b * block
        for j in range(hd_dev):
            q = S["qh"][rows(j * n * r + first, block, 16), :]
            s1 = jnp.where(pre_seen, dot_t(q, S["kall"][:prefix, :]) * scale, NEG)
            s2 = jnp.where(new_seen, dot_t(q, S["kall"][prefix:, :]) * scale, NEG)
            top = jnp.maximum(jnp.max(s1, axis=1, keepdims=True), jnp.max(s2, axis=1, keepdims=True))
            p1 = jnp.exp(s1 - top)
            p2 = jnp.exp(s2 - top)
            den = jnp.sum(p1, axis=1, keepdims=True) + jnp.sum(p2, axis=1, keepdims=True)
            o = (dot(p1.astype(BF16), S["vall"][:prefix, :]) + dot(p2.astype(BF16), S["vall"][prefix:, :])) / den
            wanted = jnp.where(row_in >= span, device * 16 + j * dec + row_in - span, -1)
            own = dot((from_col == wanted).astype(BF16), S["decr"][...].reshape(n * 16, HD))
            S["att"][k, rows(first, block, 16), j * HD : (j + 1) * HD] = jnp.where(
                row_in < span, o, own
            ).astype(BF16)
        return carry

    lax.fori_loop(0, n // block_devs, attend, 0)
    att_copy = copies.start(remote(
        S["att"].at[k], S["att"].at[k], S["x_s"].at[3], S["x_r"].at[3], **{CORE: other},
    ))
    l_w.wait()
    wo_copy.wait_recv()
    att_copy.wait_recv()

    width = 256

    def project(i, carry):
        at = cols(i * width, width)
        S["part"][:, at] = dot(S["att"][0], S["wo"][0, :, at]) + dot(S["att"][1], S["wo"][1, :, at])
        return carry

    lax.fori_loop(0, half // width, project, 0)
    quarter = half // 2

    def share(dest, h, sub):
        return S["part"][rows(dest * 2 * r, 2 * r, 16), h * quarter : (h + 1) * quarter]

    total = ring_reduce(y, c, copies, share, S["rs_out"], S["rs_in"], S["rs_s"], S["rs_r"], 1)
    return [total(h, 0) for h in range(2)]


def entry_barrier(y, k, chips, x=None, groups=0):
    def greet():
        barrier = pltpu.get_barrier_semaphore()
        for o in range(chips):
            for kk in ([1] if o == 0 else [0, 1]):
                pl.semaphore_signal(
                    barrier, inc=1,
                    device_id={CHIP: lax.rem(y + o, chips), CORE: lax.rem(k + kk, 2)},
                    device_id_type=MESH,
                )
        for o in range(1, groups):
            pl.semaphore_signal(
                barrier, inc=1, device_id={EXP: lax.rem(x + o, groups)}, device_id_type=MESH
            )
        pl.semaphore_wait(barrier, 2 * chips - 1 + max(groups - 1, 0))

    return greet


def k1_only(d, names, *refs):
    q, nkv, pre, dec, plen, dlen, wo, out, *rest = refs
    S = dict(zip(names, rest))
    y, k = lax.axis_index(CHIP), lax.axis_index(CORE)
    copies = Copies()
    got = attend_and_project(d, S, y, k, copies, q, nkv, pre, dec, plen, dlen, wo, entry_barrier(y, k, d["chips"]))
    r = d["rows"]
    mine = jnp.concatenate(got, axis=1)
    S["fin"][k] = mine
    copy = copies.start(remote(S["fin"].at[k], S["fin"].at[k], S["x_s"].at[4], S["x_r"].at[4], **{CORE: 1 - k}))
    copy.wait_recv()
    half = d["model"] // 2
    out[:, :half] = S["fin"][0, rows(k * r, r, 8), :]
    out[:, half:] = S["fin"][1, rows(k * r, r, 8), :]
    copies.drain()


def dims(hidden_in, queries, new_kv, prefix_kv, decode_kv, decode_len):
    kvw = new_kv.shape[2]
    chips = lax.axis_size(CHIP)
    hq = queries.shape[1] // HD
    return dict(
        rows=hidden_in.shape[0], model=hidden_in.shape[1], kvw=kvw, chips=chips, heads_q=hq,
        per_kv=hq // (kvw // HD), heads_dev=hq // (2 * chips), pre_dev=prefix_kv.shape[2],
        dec=decode_len.shape[0], ctx=decode_kv.shape[2],
    )


def run_k1(d, queries, new_kv, prefix_kv, decode_kv, prefix_len, decode_len, out_proj):
    scratch = k1_scratch(d)
    scratch["fin"] = pltpu.VMEM((2, 2 * d["rows"], d["model"] // 2), F32)
    names = list(scratch)
    anys = pl.BlockSpec(memory_space=pl.ANY)
    smem = pl.BlockSpec(memory_space=pltpu.SMEM)

    def kernel(*refs):
        k1_only(d, names, *refs)

    return pl.pallas_call(
        kernel,
        out_shape=jax.ShapeDtypeStruct((d["rows"], d["model"]), F32),
        in_specs=[anys] * 4 + [smem] * 2 + [anys],
        out_specs=pl.BlockSpec(memory_space=pltpu.VMEM),
        scratch_shapes=list(scratch.values()),
        compiler_params=pltpu.CompilerParams(collective_id=0, has_side_effects=True),
        name="attend",
    )(queries, new_kv, prefix_kv, decode_kv, prefix_len, decode_len, out_proj)


def on_device(
    hidden_in,
    queries,
    new_kv,
    prefix_kv,
    decode_kv,
    prefix_len,
    decode_len,
    out_proj,
    norm_gain,
    router_w,
    expert_ids,
    w_gate,
    w_up,
    w_down,
):
    groups = lax.axis_size("exp")
    rows_dev, model_width = hidden_in.shape
    d = dims(hidden_in, queries, new_kv, prefix_kv, decode_kv, decode_len)
    projected = run_k1(d, queries, new_kv, prefix_kv, decode_kv, prefix_len, decode_len, out_proj)
    residual = hidden_in.astype(jnp.float32) + projected
    mean_square = jnp.mean(residual * residual, axis=1, keepdims=True)
    normed = (residual * lax.rsqrt(mean_square + 1e-05) * norm_gain).astype(jnp.bfloat16)
    logits = jnp.dot(normed, router_w, preferred_element_type=jnp.float32)
    experts = router_w.shape[1]
    chosen_hot = (expert_ids[:, :, None] == jnp.arange(experts, dtype=jnp.int32)).astype(jnp.int32)
    chosen_logits = jnp.sum(jnp.where(chosen_hot == 1, logits[:, None, :], 0.0), axis=2)
    route_weights = jax.nn.softmax(chosen_logits, axis=1)
    flat_hot = chosen_hot.reshape(rows_dev * 2, experts)
    slot_rank = jnp.sum((jnp.cumsum(flat_hot, axis=0) - flat_hot) * flat_hot, axis=1).reshape(
        rows_dev, 2
    )
    capacity = CAP
    slot_index = jnp.arange(capacity, dtype=jnp.int32)
    assignment = chosen_hot[:, :, :, None] * (slot_rank[:, :, None, None] == slot_index).astype(
        jnp.int32
    )
    placement = jnp.sum(assignment, axis=1)
    local_experts = experts // groups
    placement_split = placement.reshape(rows_dev, groups, local_experts, capacity).astype(
        jnp.bfloat16
    )
    outgoing = jnp.einsum(
        "rnlc,rd->lncd", placement_split, normed, preferred_element_type=jnp.float32
    ).astype(jnp.bfloat16)
    arrived = lax.all_to_all(outgoing, "exp", split_axis=1, concat_axis=1, tiled=True)
    shard_rows = lax.all_gather(arrived, TEN, axis=1, tiled=True)
    gate_act = jnp.einsum("lscd,ldf->lscf", shard_rows, w_gate, preferred_element_type=jnp.float32)
    up_act = jnp.einsum("lscd,ldf->lscf", shard_rows, w_up, preferred_element_type=jnp.float32)
    hidden = (jax.nn.silu(gate_act) * up_act).astype(jnp.bfloat16)
    row_block = hidden
    summed = lax.psum_scatter(
        jnp.einsum("lscf,lfd->slcd", row_block, w_down, preferred_element_type=jnp.float32).astype(
            jnp.bfloat16
        ),
        TEN,
        scatter_dimension=0,
        tiled=True,
    )
    returned = lax.all_to_all(summed, "exp", split_axis=0, concat_axis=0, tiled=True)
    outputs = returned.reshape(experts * capacity, model_width).astype(jnp.float32)
    weight_map = jnp.sum(
        assignment.astype(jnp.float32) * route_weights[:, :, None, None], axis=1
    ).reshape(rows_dev, experts * capacity)
    expert_mix = jnp.dot(weight_map, outputs, preferred_element_type=jnp.float32)
    return (residual + expert_mix).astype(jnp.bfloat16)


def solution(mesh):
    split = Mesh(
        mesh.devices.reshape(mesh.shape["rep"], mesh.shape["exp"], mesh.shape["ten"] // 2, 2),
        ("rep", "exp", "ten_0", "ten_1"),
    )
    return jax.shard_map(
        on_device,
        mesh=split,
        in_specs=(
            P(REP_EXP_TEN, None),
            P(REP_EXP_TEN, None),
            P(None, REP_EXP_TEN, None),
            P(None, ("rep", "exp"), TEN, None),
            P(None, REP_EXP_TEN, None, None),
            P(("rep", "exp")),
            P(REP_EXP_TEN),
            P(TEN, None),
            P(),
            P(),
            P(REP_EXP_TEN, None),
            P("exp", None, TEN),
            P("exp", None, TEN),
            P("exp", TEN, None),
        ),
        out_specs=P(REP_EXP_TEN, None),
        check_vma=False,
    )
```

```python
import jax
import jax.numpy as jnp
from jax import lax
from jax.experimental import pallas as pl
from jax.experimental.pallas import tpu as pltpu
from jax.sharding import Mesh
from jax.sharding import PartitionSpec as P

MESH = pl.DeviceIdType.MESH
HD = 128
CAP = 7
F32 = jnp.float32
BF16 = jnp.bfloat16
NEG = -1e30
CHUNKS = 6
RING_WIRE, RING_TURN, RING_SPREAD = 1.25, 2.2, 4.5
EXP, CHIP, CORE = "exp", "ten_0", "ten_1"
TEN = (CHIP, CORE)
REP_EXP_TEN = ("rep", EXP, CHIP, CORE)


def iota(shape, dim):
    return lax.broadcasted_iota(jnp.int32, shape, dim)


def cols(start, size):
    return pl.ds(pl.multiple_of(start, 128), size)


def rows(start, size, align):
    return pl.ds(pl.multiple_of(start, align), size)


def dot(a, b):
    return jnp.dot(a, b, preferred_element_type=F32)


def dot_t(a, b):
    return lax.dot_general(a, b, (((1,), (1,)), ((), ())), preferred_element_type=F32)


def ring_order(chips):
    far = chips // 2
    order = []
    for hop in range(far - 1, 0, -1):
        order += [(False, hop), (True, hop + 1)]
    return order + [(True, 1)]


def ring_schedule(chips, subs, wire, turn, spread):
    order = ring_order(chips)
    place = {m: i for i, m in enumerate(order)}
    arrive, clock = {}, 0.0
    for index in (0, 1):
        for sub in range(subs):
            clock += wire
            arrive[index, sub] = clock + turn
    waiting = [(index, sub) for index in range(2, len(order)) for sub in range(subs)]
    steps = []
    while waiting:
        ready = {
            (index, sub): arrive.get((place[order[index][0], order[index][1] + 1], sub), 1e9)
            for index, sub in waiting
        }
        clock = max(clock, min(ready.values()))
        due = {m: spread * m[1] - order[m[0]][1] * (wire + turn) for m in waiting if ready[m] <= clock}
        pick = min(due, key=lambda m: (due[m], m))
        waiting.remove(pick)
        steps.append((clock, 0) + pick)
        clock += wire
        arrive[pick] = clock + turn
    last = [place[True, 1], place[False, 1]]
    for sub in range(subs):
        steps.append((max(arrive[i, sub] for i in last), 1, 0, sub))
    return [step[1:] for step in sorted(steps)]


def near_first(n):
    return [(o + 1) // 2 if o % 2 else n - o // 2 for o in range(1, n)]


def ring_turns(chips):
    far = chips // 2
    return [far] + [o for d in range(far - 1, 0, -1) for o in (d, chips - d)] + [0]


class Copies:
    def __init__(self):
        self.kinds = []

    def start(self, copy):
        copy.start()
        return copy

    def sent(self, whole, sem):
        self.kinds.append((whole, sem))

    def drain(self):
        for whole, sem in self.kinds:
            arrived(whole, sem)


def arrived(whole, sem):
    pltpu.make_async_copy(whole, whole, sem).wait()


def remote(src, dst, send_sem, recv_sem, **device):
    return pltpu.make_async_remote_copy(
        src_ref=src, dst_ref=dst, send_sem=send_sem, recv_sem=recv_sem,
        device_id=device, device_id_type=MESH,
    )


class RingSum:
    def __init__(self, y, chips, copies, part, out, into, s_sem, r_sem, subs):
        self.y, self.chips, self.copies, self.part = y, chips, copies, part
        self.out, self.into, self.s_sem, self.r_sem, self.subs = out, into, s_sem, r_sem, subs
        self.order = ring_order(chips)
        self.place = {m: i for i, m in enumerate(self.order)}
        copies.sent(out, s_sem.at[0])

    def first(self, index, sub, way, before=None):
        is_long, hop = self.order[index]
        value = self.part(hop if way == 0 else self.chips - hop, (0 if is_long else 1) ^ way, sub)
        if before is not None:
            value = value + self.into[way, before, sub].astype(F32)
        self.out[way, index, sub] = value.astype(BF16)
        to = lax.rem(self.y + (1 if way == 0 else self.chips - 1), self.chips)
        self.copies.start(remote(
            self.out.at[way, index, sub], self.into.at[way, index, sub],
            self.s_sem.at[0], self.r_sem.at[index, sub], **{CHIP: to},
        ))

    def wait(self, index, sub):
        arrived(self.into.at[:, index, sub], self.r_sem.at[index, sub])

    def send(self, index, sub):
        is_long, hop = self.order[index]
        before = self.place[is_long, hop + 1]
        self.wait(before, sub)
        for way in range(2):
            self.first(index, sub, way, before)

    def totals(self, sub):
        last = [self.place[True, 1], self.place[False, 1]]
        for index in last:
            self.wait(index, sub)
        return [
            self.part(0, half, sub)
            + self.into[0, last[half], sub].astype(F32)
            + self.into[1, last[1 - half], sub].astype(F32)
            for half in range(2)
        ]


def k1_scratch(d):
    r, c, n = d["rows"], d["chips"], 2 * d["chips"]
    jw = d["heads_dev"] * HD
    half = d["model"] // 2
    msgs = len(ring_order(c))
    v, dma = pltpu.VMEM, pltpu.SemaphoreType.DMA
    return dict(
        q_v=v((r, d["heads_q"] * HD), BF16),
        nkv_v=v((2, r, d["kvw"]), BF16),
        pre_v=v((2, d["pre_dev"], d["kvw"]), BF16),
        dec_v=v((2, d["dec"], d["ctx"], d["kvw"]), BF16),
        qb=v((n, r, jw), BF16),
        kvn=v((2, c, 2, r, HD), BF16),
        kvp=v((2, c, 2, d["pre_dev"], HD), BF16),
        dec_o=v((d["heads_q"] * 8, HD), BF16),
        decs=v((n, 16, HD), BF16),
        decr=v((n, 16, HD), BF16),
        qh=v((d["heads_dev"] * n * r, HD), BF16),
        kall=v((n * (d["pre_dev"] + r), HD), BF16),
        vall=v((n * (d["pre_dev"] + r), HD), BF16),
        att=v((n * r, 2 * jw), BF16),
        wo=v((2 * jw, half), BF16),
        part=v((n * r, half), F32),
        rs_out=v((2, msgs, CHUNKS // 2, 2 * r, half // CHUNKS), BF16),
        rs_in=v((2, msgs, CHUNKS // 2, 2 * r, half // CHUNKS), BF16),
        l_sem=dma((8,)),
        qs_sem=dma((1,)),
        qr_sem=dma((1,)),
        kns_sem=dma((1,)),
        knr_sem=dma((1,)),
        kps_sem=dma((1,)),
        kpr_sem=dma((1,)),
        x_s=dma((5,)),
        x_r=dma((5,)),
        ds_sem=dma((1,)),
        dr_sem=dma((1,)),
        rs_s=dma((1,)),
        rs_r=dma((msgs, CHUNKS // 2)),
    )


def attend_and_project(d, S, y, k, copies, q_hbm, nkv_hbm, pre_hbm, dec_hbm, plen, dlen, wo_hbm, barrier, then):
    r, c, n, dec, span = d["rows"], d["chips"], 2 * d["chips"], d["dec"], d["rows"] - d["dec"]
    hq, per_kv, hd_dev, ctx, pre_dev = d["heads_q"], d["per_kv"], d["heads_dev"], d["ctx"], d["pre_dev"]
    jw, half = hd_dev * HD, d["model"] // 2
    t = 2 * y + k
    other = 1 - k
    scale = HD ** -0.5
    l_sem = S["l_sem"]

    def local(src, dst, i):
        copy = pltpu.make_async_copy(src, dst, l_sem.at[i])
        copy.start()
        return copy

    kv_cols = cols(y * HD, HD)
    l_n = local(nkv_hbm, S["nkv_v"], 0)
    l_p = local(pre_hbm.at[:, 0], S["pre_v"], 1)
    l_q = local(q_hbm, S["q_v"], 2)
    l_own = [
        local(nkv_hbm.at[:, :, kv_cols], S["kvn"].at[k, y], 3),
        local(pre_hbm.at[:, 0, :, kv_cols], S["kvp"].at[k, y], 4),
        local(q_hbm.at[:, cols(t * jw, jw)], S["qb"].at[t], 5),
    ]
    l_d = local(dec_hbm, S["dec_v"], 6)
    l_w = local(wo_hbm.at[:, cols(k * half, half)], S["wo"].at[rows(k * jw, jw, 16)], 7)

    barrier()

    def kn_copy(src_y, to):
        return remote(
            S["nkv_v"].at[:, :, cols(to * HD, HD)], S["kvn"].at[k, src_y],
            S["kns_sem"].at[0], S["knr_sem"].at[0], **{CHIP: to},
        )

    def kp_copy(src_y, to):
        return remote(
            S["pre_v"].at[:, :, cols(to * HD, HD)], S["kvp"].at[k, src_y],
            S["kps_sem"].at[0], S["kpr_sem"].at[0], **{CHIP: to},
        )

    def q_copy(src_t, to_t):
        return remote(
            S["q_v"].at[:, cols(to_t * jw, jw)], S["qb"].at[src_t],
            S["qs_sem"].at[0], S["qr_sem"].at[0], **{CHIP: to_t // 2, CORE: to_t % 2},
        )

    l_n.wait()
    l_p.wait()
    for o in near_first(c)[::-1]:
        to = lax.rem(y + o, c)
        copies.start(kn_copy(y, to))
        copies.start(kp_copy(y, to))
    wo_copy = copies.start(remote(
        wo_hbm.at[:, cols(other * half, half)], S["wo"].at[rows(k * jw, jw, 16)], S["x_s"].at[0], S["x_r"].at[0],
        **{CORE: other},
    ))
    then()

    l_q.wait()
    l_d.wait()
    q8 = S["q_v"][16:24, :].astype(F32)
    n8 = [S["nkv_v"][i, 16:24, :].astype(F32) for i in range(2)]
    m = per_kv * 8
    keys = dec * ctx
    lane = iota((m, keys), 1)
    row8 = iota((m, keys), 0) & 7
    req = sum((lane >= ctx * i).astype(jnp.int32) for i in range(1, dec))
    pos = lane - ctx * req
    length = dlen[0]
    for i in range(1, dec):
        length = jnp.where(req == i, dlen[i], length)
    seen = (row8 - (8 - dec) == req) & (pos < length)
    for g in range(hq // per_kv):
        qg = jnp.concatenate(
            [q8[:, (g * per_kv + h) * HD : (g * per_kv + h + 1) * HD] for h in range(per_kv)], axis=0
        )
        kg = S["dec_v"][0, :, :, g * HD : (g + 1) * HD].reshape(keys, HD)
        vg = S["dec_v"][1, :, :, g * HD : (g + 1) * HD].reshape(keys, HD)
        own_k = jnp.concatenate([n8[0][:, g * HD : (g + 1) * HD]] * per_kv, axis=0)
        own_v = jnp.concatenate([n8[1][:, g * HD : (g + 1) * HD]] * per_kv, axis=0)
        s = jnp.where(seen, dot_t(qg.astype(BF16), kg) * scale, NEG)
        s_own = jnp.sum(qg * own_k, axis=1, keepdims=True) * scale
        top = jnp.maximum(jnp.max(s, axis=1, keepdims=True), s_own)
        p = jnp.where(seen, jnp.exp(s - top), 0.0)
        p_own = jnp.exp(s_own - top)
        den = jnp.sum(p, axis=1, keepdims=True) + p_own
        o = dot(p.astype(BF16), vg) + p_own.astype(BF16).astype(F32) * own_v
        S["dec_o"][g * m : (g + 1) * m, :] = (o / den).astype(BF16)
    to_row = iota((n * 16, hq * 8), 0)
    from_row = iota((n * 16, hq * 8), 1)
    slot = to_row & 15
    wanted = (to_row >> 4) * (8 * hd_dev) + (slot >> 2) * 8 + (8 - dec) + (slot & 3)
    pick = ((from_row == wanted) & (slot < hd_dev * dec)).astype(BF16)
    S["decs"][...] = dot(pick, S["dec_o"][...]).astype(BF16).reshape(n, 16, HD)

    def d_copy(src_t, to_t):
        return remote(
            S["decs"].at[to_t], S["decr"].at[src_t],
            S["ds_sem"].at[0], S["dr_sem"].at[0], **{CHIP: to_t // 2, CORE: to_t % 2},
        )

    for o in range(n - 1, 0, -1):
        copies.start(d_copy(t, lax.rem(t + o, n)))
    S["decr"][t] = S["decs"][t]
    for o in near_first(c)[::-1] + [0]:
        to = lax.rem(y + o, c)
        for kk in ([1] if o == 0 else [0, 1]):
            copies.start(q_copy(t, 2 * to + lax.rem(k + kk, 2)))

    for copy in l_own:
        copy.wait()
    arrived(S["kvn"].at[k, : c - 1], S["knr_sem"].at[0])
    arrived(S["kvp"].at[k, : c - 1], S["kpr_sem"].at[0])
    copies.sent(S["kvn"].at[k, : c - 1], S["kns_sem"].at[0])
    copies.sent(S["kvp"].at[k, : c - 1], S["kps_sem"].at[0])
    copies.sent(S["qb"].at[: n - 1], S["qs_sem"].at[0])
    copies.sent(S["decs"].at[: n - 1], S["ds_sem"].at[0])
    relay = [
        copies.start(remote(S[b].at[k], S[b].at[k], S["x_s"].at[i], S["x_r"].at[i], **{CORE: other}))
        for i, b in ((1, "kvn"), (2, "kvp"))
    ]
    arrived(S["qb"].at[: n - 1], S["qr_sem"].at[0])
    turn = ring_turns(c)
    chip_at = [lax.rem(y + o, c) for o in turn]
    for cc in range(c):
        pair = [S["qb"][2 * chip_at[cc] + i].astype(F32) for i in range(2)]
        for j in range(hd_dev):
            S["qh"][j * n * r + cc * 2 * r : j * n * r + (cc + 1) * 2 * r, :] = jnp.concatenate(
                [q[:, j * HD : (j + 1) * HD] for q in pair], axis=0
            ).astype(BF16)
    for copy in relay:
        copy.wait()
    prefix = n * pre_dev
    for i, b in ((0, "kall"), (1, "vall")):
        for cc in range(c):
            for kk in range(2):
                at = (2 * cc + kk) * pre_dev
                S[b][at : at + pre_dev, :] = S["kvp"][kk, cc, i]
            S[b][prefix + cc * 2 * r : prefix + (cc + 1) * 2 * r, :] = jnp.concatenate(
                [S["kvn"][kk, cc, i].astype(F32) for kk in range(2)], axis=0
            ).astype(BF16)
    arrived(S["decr"].at[: n - 1], S["dr_sem"].at[0])

    block_devs = 8
    block = block_devs * r
    col = iota((1, n * r), 1)
    col_dev = sum((col >= r * i).astype(jnp.int32) for i in range(1, n))
    col_in = col - r * col_dev
    key_place = jnp.where(col_in < span, col_dev * span + col_in, 1 << 20)
    pre_seen = iota((1, prefix), 1) < plen[0]
    row = iota((block, 1), 0)
    row_dev = sum((row >= r * i).astype(jnp.int32) for i in range(1, block_devs))
    row_in = row - r * row_dev
    from_col = iota((block, n * 16), 1)
    att_copies = []
    for b in range(n // block_devs):
        chip = sum(
            jnp.where((row_dev >> 1) == i, chip_at[b * block_devs // 2 + i], 0) for i in range(block_devs // 2)
        )
        device = 2 * chip + (row_dev & 1)
        new_seen = key_place <= device * span + row_in
        first = b * block
        for j in range(hd_dev):
            q = S["qh"][j * n * r + first : j * n * r + first + block, :]
            s1 = jnp.where(pre_seen, dot_t(q, S["kall"][:prefix, :]), NEG)
            s2 = jnp.where(new_seen, dot_t(q, S["kall"][prefix:, :]), NEG)
            top = jnp.maximum(jnp.max(s1, axis=1, keepdims=True), jnp.max(s2, axis=1, keepdims=True))
            p1 = jnp.exp((s1 - top) * scale)
            p2 = jnp.exp((s2 - top) * scale)
            den = jnp.sum(p1, axis=1, keepdims=True) + jnp.sum(p2, axis=1, keepdims=True)
            o = (dot(p1.astype(BF16), S["vall"][:prefix, :]) + dot(p2.astype(BF16), S["vall"][prefix:, :])) / den
            wanted = jnp.where(row_in >= span, device * 16 + j * dec + row_in - span, -1)
            own = dot((from_col == wanted).astype(BF16), S["decr"][...].reshape(n * 16, HD))
            S["att"][first : first + block, cols(k * jw + j * HD, HD)] = jnp.where(
                row_in < span, o, own
            ).astype(BF16)
        view = S["att"].at[first : first + block, cols(k * jw, jw)]
        att_copies.append(copies.start(remote(
            view, view, S["x_s"].at[3 + b], S["x_r"].at[3 + b], **{CORE: other},
        )))
    l_w.wait()
    wo_copy.wait()

    width, subs = half // CHUNKS, CHUNKS // 2
    row_of = {o: i * 2 * r for i, o in enumerate(turn)}

    def share(o, h, sub):
        first = (h * subs + sub) * width
        return S["part"][row_of[o] : row_of[o] + 2 * r, first : first + width]

    ring = RingSum(y, c, copies, share, S["rs_out"], S["rs_in"], S["rs_s"], S["rs_r"], subs)
    for b, copy in enumerate(att_copies):
        copy.wait()
        these = slice(b * block, (b + 1) * block)
        for sub in range(subs):
            for h in range(2):
                first = (h * subs + sub) * width
                S["part"][these, first : first + width] = dot(
                    S["att"][these, :], S["wo"][:, first : first + width]
                )
                if b == 0:
                    ring.first(0, sub, 1 - h)
                    ring.first(1, sub, h)
    for index in range(2, len(ring.order)):
        for sub in range(subs):
            ring.send(index, sub)
    sums = [ring.totals(sub) for sub in range(subs)]
    return [sums[sub][h] for h in range(2) for sub in range(subs)]


def entry_barrier(y, k, chips, x=None, groups=0):
    def greet():
        barrier = pltpu.get_barrier_semaphore()
        for o in range(chips):
            for kk in ([1] if o == 0 else [0, 1]):
                pl.semaphore_signal(
                    barrier, inc=1,
                    device_id={CHIP: lax.rem(y + o, chips), CORE: lax.rem(k + kk, 2)},
                    device_id_type=MESH,
                )
        for o in range(1, groups):
            pl.semaphore_signal(
                barrier, inc=1, device_id={EXP: lax.rem(x + o, groups)}, device_id_type=MESH
            )
        pl.semaphore_wait(barrier, 2 * chips - 1 + max(groups - 1, 0))

    return greet


def moe_scratch(d):
    r, c, groups, model, ff = d["rows"], d["chips"], d["groups"], d["model"], d["ff_dev"]
    half, slots, take = model // 2, 16, 2 * CAP
    far, nq, msgs = c // 2, CHUNKS, len(ring_order(c))
    v, dma = pltpu.VMEM, pltpu.SemaphoreType.DMA
    return dict(
        ids_v=v((2, r), jnp.int32),
        gain_v=v((1, model), F32),
        router_v=v((d["experts"], model), BF16),
        ids_b=v((2, r, 128), jnp.int32),
        hin=v((2, r, half), BF16),
        res=v((2 * r, half), F32),
        stat=v((2, 2 * r, 128), F32),
        pick=v((2, 2 * r, 128), F32),
        normed=v((2 * r, half), BF16),
        wg=v((model, ff), BF16),
        wu=v((model, ff), BF16),
        wd=v((2, ff, half), BF16),
        xs=v((groups, slots, half), BF16),
        xr=v((groups, slots, half), BF16),
        xg=v((2, c, groups * take, half), BF16),
        hid=v((2, c * groups * take, ff), BF16),
        part2=v((c * groups * take, half), F32),
        rs2_out=v((2, msgs, nq // 2, groups * take, half // nq), BF16),
        rs2_in=v((2, msgs, nq // 2, groups * take, half // nq), BF16),
        ys=v((groups, slots, half), BF16),
        yr=v((groups, slots, half), BF16),
        fin=v((2, 2 * r, half), F32),
        m_l=dma((8,)),
        m_s=dma((5,)),
        m_r=dma((5,)),
        xs_s=dma((1,)),
        xs_r=dma((nq,)),
        ag_s=dma((1,)),
        ag_r=dma((far, nq)),
        pc_s=dma((1,)),
        pc_r=dma((far + 1,)),
        h_s=dma((1,)),
        h_r=dma((far + 1,)),
        rs2_s=dma((1,)),
        rs2_r=dma((msgs, nq // 2)),
        ys_s=dma((1,)),
        ys_r=dma((nq,)),
        f_s=dma((1,)),
        f_r=dma((1,)),
    )


class Experts:
    def __init__(self, d, S, x, y, k, copies, hidden_hbm, ids, gain, router_t, wg_hbm, wu_hbm, wd_hbm, out):
        self.d, self.S, self.x, self.y, self.k, self.copies = d, S, x, y, k, copies
        self.hidden_hbm, self.ids, self.gain, self.router_t = hidden_hbm, ids, gain, router_t
        self.wg_hbm, self.wu_hbm, self.wd_hbm, self.out = wg_hbm, wu_hbm, wd_hbm, out

    def early(self):
        self.ids_load = pltpu.make_async_copy(self.ids, self.S["ids_v"], self.S["m_l"].at[4])
        self.ids_load.start()

    def load(self):
        S, k, d = self.S, self.k, self.d
        half, other = d["model"] // 2, 1 - self.k
        r = d["rows"]
        self.ids_load.wait()
        one = (iota((r, r), 0) == iota((r, r), 1)).astype(BF16)
        ids = dot_t(one, S["ids_v"][...].astype(F32).astype(BF16)).astype(jnp.int32)
        lane = iota((r, 128), 1)
        S["ids_b"][k] = jnp.where(lane < 64, ids[:, 0:1], ids[:, 1:2])

        def exchange(src, dst, i):
            return self.copies.start(remote(src, dst, S["m_s"].at[i], S["m_r"].at[i], **{CORE: other}))

        self.ids_copy = exchange(S["ids_b"].at[k], S["ids_b"].at[k], 0)
        self.hin_copy = exchange(self.hidden_hbm.at[:, cols(other * half, half)], S["hin"].at[k], 1)
        self.wd_copy = exchange(self.wd_hbm.at[0, :, cols(other * half, half)], S["wd"].at[k], 2)
        self.exchange = exchange
        self.loads = []
        for i, (src, dst) in enumerate((
            (self.hidden_hbm.at[:, cols(k * half, half)], S["hin"].at[k]),
            (self.wg_hbm.at[0], S["wg"]),
            (self.wu_hbm.at[0], S["wu"]),
            (self.wd_hbm.at[0, :, cols(k * half, half)], S["wd"].at[k]),
            (self.gain, S["gain_v"]),
            (self.router_t, S["router_v"]),
        )):
            copy = pltpu.make_async_copy(src, dst, S["m_l"].at[i if i < 4 else i + 1])
            copy.start()
            self.loads.append(copy)

    def away(self, o):
        return min(o, self.d["chips"] - o)

    def chip(self, o):
        return self.y if o == 0 else lax.rem(self.y + o, self.d["chips"])

    def route(self):
        S, d = self.S, self.d
        r = d["rows"]
        self.ids_copy.wait()
        ids = S["ids_b"][...].reshape(2 * r, 128)
        lane, row = iota((2 * r, 128), 1), iota((2 * r, 128), 0)
        expert, slot = lane >> 4, lane & 15
        self.first = ids[:, 0:1] == expert
        hot = self.first | (ids[:, 64:65] == expert)
        a, b = iota((2 * r, 2 * r), 0), iota((2 * r, 2 * r), 1)
        below = ((b < a) & ((a < r) == (b < r))).astype(BF16)
        rank = dot(below, hot.astype(BF16)).astype(jnp.int32) + jnp.where(row < r, 0, CAP)
        self.placed = hot & (rank == slot)
        one = (iota((128, 128), 0) == iota((128, 128), 1)).astype(BF16)
        self.to_slots = dot_t(one, self.placed.astype(BF16)).astype(BF16)
        self.ids2 = ids
        self.hin_copy.wait()
        for i in (0, 4, 5):
            self.loads[i].wait()

    def ffn_gate_up(self, offs, tile):
        S, d = self.S, self.d
        half, n = d["model"] // 2, d["groups"] * 2 * CAP
        width = d["ff_dev"] // 2
        at = slice(tile * width, (tile + 1) * width)
        xh = [jnp.concatenate([S["xg"][h, self.chip(o)] for o in offs], axis=0) for h in range(2)]
        gate = dot(xh[0], S["wg"][:half, at]) + dot(xh[1], S["wg"][half:, at])
        up = dot(xh[0], S["wu"][:half, at]) + dot(xh[1], S["wu"][half:, at])
        act = (gate / (1.0 + jnp.exp(-gate)) * up).astype(BF16)
        for i, o in enumerate(offs):
            S["hid"][self.k, rows(self.chip(o) * n, n, 16), at] = act[i * n : (i + 1) * n]

    def hid_copy(self, o):
        n = self.d["groups"] * 2 * CAP
        view = self.S["hid"].at[self.k, rows(self.chip(o) * n, n, 16)]
        return remote(view, view, self.S["h_s"].at[0], self.S["h_r"].at[self.away(o)], **{CORE: 1 - self.k})

    def ffn_down(self, offs, after=None):
        S, d = self.S, self.d
        half, n = d["model"] // 2, d["groups"] * 2 * CAP
        lhs = [
            jnp.concatenate([S["hid"][h, rows(self.chip(o) * n, n, 16), :] for o in offs], axis=0)
            for h in range(2)
        ]

        def tile(at):
            value = dot(lhs[0], S["wd"][0, :, at]) + dot(lhs[1], S["wd"][1, :, at])
            for j, o in enumerate(offs):
                S["part2"][rows(self.chip(o) * n, n, 16), at] = value[j * n : (j + 1) * n]

        def step(i, carry):
            tile(cols(i * 256, 256))
            return carry

        width, subs = half // CHUNKS, CHUNKS // 2
        if after is None:
            lax.fori_loop(0, half // 256, step, 0)
        else:
            for sub in range(subs):
                for h in range(2):
                    first = (h * subs + sub) * width
                    tile(slice(first, first + width))
                    after(h, sub)

    def ffn(self, offs, stage, after=None):
        if stage == 0:
            arrived(self.S["xg"].at[0, : len(offs)], self.S["pc_r"].at[self.away(offs[0])])
            self.ffn_gate_up(offs, 0)
        elif stage == 1:
            self.ffn_gate_up(offs, 1)
            for o in offs:
                self.copies.start(self.hid_copy(o))
        elif stage == CHUNKS - 1:
            n = self.d["groups"] * 2 * CAP
            arrived(self.S["hid"].at[0, : len(offs) * n], self.S["h_r"].at[self.away(offs[0])])
            self.ffn_down(offs, after)

    def chunk(self, q):
        w = self.d["model"] // 2 // CHUNKS
        return slice(q * w, (q + 1) * w)

    def partner_copy(self, o, q):
        S = self.S
        view = S["xg"].at[self.k, self.chip(o), :, self.chunk(q)]
        return remote(view, view, S["pc_s"].at[0], S["pc_r"].at[self.away(o)], **{CORE: 1 - self.k})

    def hops(self, way, q):
        far = self.d["chips"] // 2
        return far if ((q // (CHUNKS // 2)) ^ way) == 0 else far - 1

    def gather_copy(self, way, hop, q):
        S, c = self.S, self.d["chips"]
        back = hop - 1
        src = self.chip((c - back) % c if way == 0 else back % c)
        to = self.chip(1 if way == 0 else c - 1)
        view = S["xg"].at[self.k, src, :, self.chunk(q)]
        return remote(view, view, S["ag_s"].at[0], S["ag_r"].at[hop - 1, q], **{CHIP: to})

    def swap(self, send, recv, s_sem, r_sem, src_x, to_x, q):
        S = self.S
        return remote(
            S[send].at[to_x, :, self.chunk(q)], S[recv].at[src_x, :, self.chunk(q)],
            S[s_sem].at[0], S[r_sem].at[q], **{EXP: to_x},
        )

    def run(self, totals):
        S, d, x, y, k, copies = self.S, self.d, self.x, self.y, self.k, self.copies
        r, c, groups, model = d["rows"], d["chips"], d["groups"], d["model"]
        half, far, n = model // 2, c // 2, groups * 2 * CAP
        w = half // CHUNKS
        res = S["hin"][...].astype(F32).reshape(2 * r, half) + jnp.concatenate(totals, axis=1)
        S["res"][...] = res
        S["stat"][k] = jnp.broadcast_to(jnp.sum(res * res, axis=1, keepdims=True), (2 * r, 128))
        stat_copy = self.exchange(S["stat"].at[k], S["stat"].at[k], 3)
        stat_copy.wait()
        mean = (S["stat"][0][:, 0:1] + S["stat"][1][:, 0:1]) / model
        gain = S["gain_v"][:, cols(k * half, half)]
        S["normed"][...] = (S["res"][...] * lax.rsqrt(mean + 1e-05) * gain).astype(BF16)

        near = [lax.rem(x + o, groups) for o in near_first(groups)[::-1]]
        for q in range(CHUNKS):
            at = self.chunk(q)
            S["xs"][:, :, at] = dot(self.to_slots, S["normed"][:, at]).astype(BF16).reshape(groups, 16, w)
            for to in near:
                copies.start(self.swap("xs", "xr", "xs_s", "xs_r", x, to, q))
        S["xr"][x] = S["xs"][x]
        normed = S["normed"][...]
        logits = dot_t(normed, S["router_v"][:, cols(k * half, half)])
        e8 = iota(logits.shape, 1)
        ids = self.ids2
        lane = iota((2 * r, 128), 1)
        chosen = [
            jnp.sum(jnp.where(e8 == ids[:, 64 * i : 64 * i + 1], logits, 0.0), axis=1, keepdims=True)
            for i in range(2)
        ]
        S["pick"][k] = jnp.where(lane < 64, chosen[0], chosen[1])
        pick_copy = self.exchange(S["pick"].at[k], S["pick"].at[k], 4)

        ja, jb = iota((n, 128), 1), iota((n, 128), 0)
        dense = (((ja >> 4) * (2 * CAP) + (ja & 15) == jb) & ((ja & 15) < 2 * CAP)).astype(BF16)
        def pass_on(hop, q):
            ways = [way for way in range(2) if hop <= self.hops(way, q)]
            arrived(S["xg"].at[k, : len(ways), :, self.chunk(q)], S["ag_r"].at[hop - 1, q])
            for way in ways:
                if hop < self.hops(way, q):
                    copies.start(self.gather_copy(way, hop + 1, q))
            for way in ways:
                copies.start(self.partner_copy(c - hop if way == 0 else hop, q))

        ahead = 2
        for q in range(CHUNKS):
            at = self.chunk(q)
            arrived(S["xr"].at[: groups - 1, :, at], S["xs_r"].at[q])
            S["xg"][k, y, :, at] = dot(dense, S["xr"][:, :, at].reshape(groups * 16, w)).astype(BF16)
            for way in range(2):
                copies.start(self.gather_copy(way, 1, q))
            copies.start(self.partner_copy(0, q))
            if q >= ahead:
                pass_on(1, q - ahead)
        for load in self.loads[1:4]:
            load.wait()
        self.wd_copy.wait()

        quarter, subs = half // CHUNKS, CHUNKS // 2

        def share(o, h, sub):
            first = (h * subs + sub) * quarter
            return S["part2"][rows(self.chip(o) * n, n, 16), first : first + quarter]

        ring = RingSum(y, c, copies, share, S["rs2_out"], S["rs2_in"], S["rs2_s"], S["rs2_r"], subs)
        blocks = [[0]] + [[c - s, s] for s in range(1, far)] + [[far]]
        for hop in range(1, far + 1):
            for q in range(CHUNKS):
                if hop > 1 or q >= CHUNKS - ahead:
                    pass_on(hop, q)
                self.ffn(
                    blocks[hop - 1], q, None if hop < far else lambda h, sub: ring.first(0, sub, 1 - h)
                )
        for stage in range(CHUNKS):
            self.ffn(blocks[far], stage, lambda h, sub: ring.first(1, sub, h))

        pick_copy.wait()
        l0 = S["pick"][0][:, 0:1] + S["pick"][1][:, 0:1]
        l1 = S["pick"][0][:, 64:65] + S["pick"][1][:, 64:65]
        top = jnp.maximum(l0, l1)
        e0, e1 = jnp.exp(l0 - top), jnp.exp(l1 - top)
        weight = jnp.where(self.placed, jnp.where(self.first, e0, e1) / (e0 + e1), 0.0)
        w_hi = weight.astype(BF16)
        w_lo = (weight - w_hi.astype(F32)).astype(BF16)
        ja, jb = iota((128, n), 0), iota((128, n), 1)
        spread = (((ja >> 4) * (2 * CAP) + (ja & 15) == jb) & ((ja & 15) < 2 * CAP)).astype(BF16)
        for kind, index, sub in ring_schedule(c, subs, RING_WIRE, RING_TURN, RING_SPREAD):
            if kind == 0:
                ring.send(index, sub)
                continue
            for h, value in enumerate(ring.totals(sub)):
                q = h * subs + sub
                at = self.chunk(q)
                S["ys"][:, :, at] = dot(spread, value.astype(BF16)).astype(BF16).reshape(groups, 16, w)
                for to in near:
                    copies.start(self.swap("ys", "yr", "ys_s", "ys_r", x, to, q))
        S["yr"][x] = S["ys"][x]

        def back(q):
            view = S["fin"].at[k, rows((1 - k) * r, r, 8), self.chunk(q)]
            return remote(view, view, S["f_s"].at[0], S["f_r"].at[0], **{CORE: 1 - k})

        for q in [h * subs + sub for sub in range(subs) for h in range(2)]:
            at = self.chunk(q)
            arrived(S["yr"].at[: groups - 1, :, at], S["ys_r"].at[q])
            got = S["yr"][:, :, at].reshape(groups * 16, w)
            S["fin"][k, :, at] = S["res"][:, at] + dot(w_hi, got) + dot(w_lo, got)
            copies.start(back(q))
        arrived(S["fin"].at[1 - k, rows(k * r, r, 8), :], S["f_r"].at[0])
        for h in range(2):
            self.out[:, h * half : (h + 1) * half] = S["fin"][h, rows(k * r, r, 8), :].astype(BF16)
        copies.sent(S["xs"].at[: groups - 1], S["xs_s"].at[0])
        copies.sent(S["ys"].at[: groups - 1], S["ys_s"].at[0])
        copies.sent(S["xg"].at[0, : c - 1], S["ag_s"].at[0])
        copies.sent(S["xg"].at[0], S["pc_s"].at[0])
        copies.sent(S["hid"].at[0], S["h_s"].at[0])
        copies.sent(S["fin"].at[k, rows((1 - k) * r, r, 8), :], S["f_s"].at[0])


def on_device(
    hidden_in,
    queries,
    new_kv,
    prefix_kv,
    decode_kv,
    prefix_len,
    decode_len,
    out_proj,
    norm_gain,
    router_w,
    expert_ids,
    w_gate,
    w_up,
    w_down,
):
    chips, hq, kvw = lax.axis_size(CHIP), queries.shape[1] // HD, new_kv.shape[2]
    d = dict(
        rows=hidden_in.shape[0], model=hidden_in.shape[1], kvw=kvw, chips=chips, heads_q=hq,
        per_kv=hq // (kvw // HD), heads_dev=hq // (2 * chips), pre_dev=prefix_kv.shape[2],
        dec=decode_len.shape[0], ctx=decode_kv.shape[2], groups=lax.axis_size(EXP), ff_dev=w_gate.shape[2],
        experts=router_w.shape[1],
    )
    scratch = {**k1_scratch(d), **moe_scratch(d)}
    names = list(scratch)

    def kernel(q, nkv, pre, dec, plen, dlen, wo, hid, ids, gain, router, wg, wu, wd, out, *rest):
        S = dict(zip(names, rest))
        x, y, k = lax.axis_index(EXP), lax.axis_index(CHIP), lax.axis_index(CORE)
        copies = Copies()
        experts = Experts(d, S, x, y, k, copies, hid, ids, gain, router, wg, wu, wd, out)
        experts.early()
        totals = attend_and_project(
            d, S, y, k, copies, q, nkv, pre, dec, plen, dlen, wo,
            entry_barrier(y, k, chips, x, d["groups"]), experts.load,
        )
        experts.route()
        experts.run(totals)
        copies.drain()

    anys = pl.BlockSpec(memory_space=pl.ANY)
    smem = pl.BlockSpec(memory_space=pltpu.SMEM)
    vmem = pl.BlockSpec(memory_space=pltpu.VMEM)
    return pl.pallas_call(
        kernel,
        out_shape=jax.ShapeDtypeStruct(hidden_in.shape, BF16),
        in_specs=[anys] * 4 + [smem] * 2 + [anys] * 8,
        out_specs=vmem,
        scratch_shapes=list(scratch.values()),
        compiler_params=pltpu.CompilerParams(collective_id=0, has_side_effects=True),
        name="layer",
    )(
        queries, new_kv, prefix_kv, decode_kv, prefix_len, decode_len, out_proj, hidden_in, expert_ids.T,
        norm_gain.reshape(1, -1), router_w.T, w_gate, w_up, w_down,
    )


def solution(mesh):
    split = Mesh(
        mesh.devices.reshape(mesh.shape["rep"], mesh.shape["exp"], mesh.shape["ten"] // 2, 2),
        ("rep", "exp", "ten_0", "ten_1"),
    )
    return jax.shard_map(
        on_device,
        mesh=split,
        in_specs=(
            P(REP_EXP_TEN, None),
            P(REP_EXP_TEN, None),
            P(None, REP_EXP_TEN, None),
            P(None, ("rep", "exp"), TEN, None),
            P(None, REP_EXP_TEN, None, None),
            P(("rep", "exp")),
            P(REP_EXP_TEN),
            P(TEN, None),
            P(),
            P(),
            P(REP_EXP_TEN, None),
            P("exp", None, TEN),
            P("exp", None, TEN),
            P("exp", TEN, None),
        ),
        out_specs=P(REP_EXP_TEN, None),
        check_vma=False,
    )
```

```python
import jax
import jax.numpy as jnp
from jax import lax
from jax.experimental import pallas as pl
from jax.experimental.pallas import tpu as pltpu
from jax.sharding import Mesh
from jax.sharding import PartitionSpec as P

MESH = pl.DeviceIdType.MESH
HD = 128
CAP = 7
F32 = jnp.float32
BF16 = jnp.bfloat16
NEG = -1e30
CHUNKS = 6
PIECES = 12
RING_WIRE, RING_TURN, RING_SPREAD, RING_LATE = 1.25, 3.2, 5.0, 2.0
EXP, CHIP, CORE = "exp", "ten_0", "ten_1"
TEN = (CHIP, CORE)
REP_EXP_TEN = ("rep", EXP, CHIP, CORE)


def iota(shape, dim):
    return lax.broadcasted_iota(jnp.int32, shape, dim)


def cols(start, size):
    return pl.ds(pl.multiple_of(start, 128), size)


def rows(start, size, align):
    return pl.ds(pl.multiple_of(start, align), size)


def dot(a, b):
    return jnp.dot(a, b, preferred_element_type=F32)


def dot_t(a, b):
    return lax.dot_general(a, b, (((1,), (1,)), ((), ())), preferred_element_type=F32)


def ring_order(chips):
    far = chips // 2
    order = []
    for hop in range(far - 1, 0, -1):
        order += [(False, hop), (True, hop + 1)]
    return order + [(True, 1)]


def ring_schedule(chips, subs, wire, turn, spread, late):
    order = ring_order(chips)
    place = {m: i for i, m in enumerate(order)}
    arrive, clock = {}, 0.0
    for index in (0, 1):
        clock = max(clock, 4.0 * index)
        for sub in range(subs):
            clock += wire
            arrive[index, sub] = clock + turn
    waiting = [(index, sub) for index in range(2, len(order)) for sub in range(subs)]
    steps = []
    while waiting:
        ready = {
            (index, sub): arrive.get((place[order[index][0], order[index][1] + 1], sub), 1e9)
            for index, sub in waiting
        }
        clock = max(clock, min(ready.values()))
        due = {m: spread * m[1] - order[m[0]][1] * (wire + turn) for m in waiting if ready[m] <= clock}
        pick = min(due, key=lambda m: (due[m], m))
        waiting.remove(pick)
        steps.append((clock, 0) + pick)
        clock += wire
        arrive[pick] = clock + turn
    last = [place[True, 1], place[False, 1]]
    for sub in range(subs):
        steps.append((max(arrive[i, sub] for i in last) + late, 1, 0, sub))
    return [step[1:] for step in sorted(steps)]


def near_first(n):
    return [(o + 1) // 2 if o % 2 else n - o // 2 for o in range(1, n)]


def ring_turns(chips):
    far = chips // 2
    return [far] + [o for d in range(far - 1, 0, -1) for o in (d, chips - d)] + [0]


class Copies:
    def __init__(self):
        self.kinds = []

    def start(self, copy):
        copy.start()
        return copy

    def sent(self, whole, sem):
        self.kinds.append((whole, sem))

    def drain(self):
        for whole, sem in self.kinds:
            arrived(whole, sem)


def arrived(whole, sem):
    pltpu.make_async_copy(whole, whole, sem).wait()


def remote(src, dst, send_sem, recv_sem, **device):
    return pltpu.make_async_remote_copy(
        src_ref=src, dst_ref=dst, send_sem=send_sem, recv_sem=recv_sem,
        device_id=device, device_id_type=MESH,
    )


class RingSum:
    def __init__(self, y, chips, copies, part, out, into, s_sem, r_sem, subs):
        self.y, self.chips, self.copies, self.part = y, chips, copies, part
        self.out, self.into, self.s_sem, self.r_sem, self.subs = out, into, s_sem, r_sem, subs
        self.order = ring_order(chips)
        self.place = {m: i for i, m in enumerate(self.order)}
        copies.sent(out, s_sem.at[0])

    def first(self, index, sub, way, before=None):
        is_long, hop = self.order[index]
        value = self.part(hop if way == 0 else self.chips - hop, (0 if is_long else 1) ^ way, sub)
        if before is not None:
            value = value + self.into[way, before, sub].astype(F32)
        self.out[way, index, sub] = value.astype(BF16)
        to = lax.rem(self.y + (1 if way == 0 else self.chips - 1), self.chips)
        self.copies.start(remote(
            self.out.at[way, index, sub], self.into.at[way, index, sub],
            self.s_sem.at[0], self.r_sem.at[index, sub], **{CHIP: to},
        ))

    def wait(self, index, sub):
        arrived(self.into.at[:, index, sub], self.r_sem.at[index, sub])

    def send(self, index, sub):
        is_long, hop = self.order[index]
        before = self.place[is_long, hop + 1]
        self.wait(before, sub)
        for way in range(2):
            self.first(index, sub, way, before)

    def totals(self, sub):
        last = [self.place[True, 1], self.place[False, 1]]
        for index in last:
            self.wait(index, sub)
        return [
            self.part(0, half, sub)
            + self.into[0, last[half], sub].astype(F32)
            + self.into[1, last[1 - half], sub].astype(F32)
            for half in range(2)
        ]


def k1_scratch(d):
    r, c, n = d["rows"], d["chips"], 2 * d["chips"]
    jw = d["heads_dev"] * HD
    half = d["model"] // 2
    msgs = len(ring_order(c))
    v, dma = pltpu.VMEM, pltpu.SemaphoreType.DMA
    return dict(
        q_v=v((r, d["heads_q"] * HD), BF16),
        nkv_v=v((2, r, d["kvw"]), BF16),
        pre_v=v((2, d["pre_dev"], d["kvw"]), BF16),
        dec_v=v((2, d["dec"], d["ctx"], d["kvw"]), BF16),
        qb=v((n, r - 8, jw), BF16),
        plen_v=v((1, 1), jnp.int32),
        kvn=v((2, c, 2, r, HD), BF16),
        kvp=v((2, c, 2, d["pre_dev"], HD), BF16),
        decs=v((n, 8 * d["heads_dev"], HD), BF16),
        decr=v((n, 8 * d["heads_dev"], HD), BF16),
        qh=v((d["heads_dev"] * n * r, HD), BF16),
        kall=v((n * (d["pre_dev"] + r), HD), BF16),
        vall=v((n * (d["pre_dev"] + r), HD), BF16),
        att=v((n * r, 2 * jw), BF16),
        wo=v((2 * jw, half), BF16),
        part=v((n * r, half), F32),
        rs_out=v((2, msgs, PIECES // 2, 2 * r, half // PIECES), BF16),
        rs_in=v((2, msgs, PIECES // 2, 2 * r, half // PIECES), BF16),
        l_sem=dma((9,)),
        qs_sem=dma((1,)),
        qr_sem=dma((2,)),
        kns_sem=dma((1,)),
        knr_sem=dma((1,)),
        kps_sem=dma((1,)),
        kpr_sem=dma((1,)),
        x_s=dma((5,)),
        x_r=dma((5,)),
        ds_sem=dma((1,)),
        dr_sem=dma((1,)),
        rs_s=dma((1,)),
        rs_r=dma((msgs, PIECES // 2)),
    )


def attend_and_project(d, S, y, k, copies, q_hbm, nkv_hbm, pre_hbm, dec_hbm, plen, dlen, wo_hbm, barrier, then):
    r, c, n, dec, span = d["rows"], d["chips"], 2 * d["chips"], d["dec"], d["rows"] - d["dec"]
    hq, per_kv, hd_dev, ctx, pre_dev = d["heads_q"], d["per_kv"], d["heads_dev"], d["ctx"], d["pre_dev"]
    jw, half = hd_dev * HD, d["model"] // 2
    t = 2 * y + k
    other = 1 - k
    scale = HD ** -0.5
    l_sem = S["l_sem"]

    def local(src, dst, i):
        copy = pltpu.make_async_copy(src, dst, l_sem.at[i])
        copy.start()
        return copy

    kv_cols = cols(y * HD, HD)
    turn = ring_turns(c)
    l_n = local(nkv_hbm, S["nkv_v"], 0)
    l_p = local(pre_hbm.at[:, 0], S["pre_v"], 1)
    l_q = local(q_hbm, S["q_v"], 2)
    l_own = [
        local(nkv_hbm.at[:, :, kv_cols], S["kvn"].at[k, y], 3),
        local(pre_hbm.at[:, 0, :, kv_cols], S["kvp"].at[k, y], 4),
        local(q_hbm.at[: r - 8, cols(t * jw, jw)], S["qb"].at[t], 5),
    ]
    l_len = local(plen, S["plen_v"], 8)
    l_d = local(dec_hbm, S["dec_v"], 6)
    l_w = local(wo_hbm.at[:, cols(k * half, half)], S["wo"].at[rows(k * jw, jw, 16)], 7)

    barrier()

    def kn_copy(src_y, to):
        return remote(
            S["nkv_v"].at[:, :, cols(to * HD, HD)], S["kvn"].at[k, src_y],
            S["kns_sem"].at[0], S["knr_sem"].at[0], **{CHIP: to},
        )

    def kp_copy(src_y, to):
        return remote(
            S["pre_v"].at[:, :, cols(to * HD, HD)], S["kvp"].at[k, src_y],
            S["kps_sem"].at[0], S["kpr_sem"].at[0], **{CHIP: to},
        )

    def q_copy(src_t, to_t, late):
        return remote(
            S["q_v"].at[: r - 8, cols(to_t * jw, jw)], S["qb"].at[src_t],
            S["qs_sem"].at[0], S["qr_sem"].at[late], **{CHIP: to_t // 2, CORE: to_t % 2},
        )

    l_n.wait()
    l_p.wait()
    for o in near_first(c)[::-1]:
        to = lax.rem(y + o, c)
        copies.start(kn_copy(y, to))
        copies.start(kp_copy(y, to))
    wo_copy = copies.start(remote(
        wo_hbm.at[:, cols(other * half, half)], S["wo"].at[rows(k * jw, jw, 16)], S["x_s"].at[0], S["x_r"].at[0],
        **{CORE: other},
    ))
    then()

    l_q.wait()
    l_d.wait()
    q8 = S["q_v"][16:24, :].astype(F32)
    n8 = [S["nkv_v"][i, 16:24, :].astype(F32) for i in range(2)]
    m = per_kv * 8
    keys = dec * ctx
    lane = iota((m, keys), 1)
    row8 = iota((m, keys), 0) & 7
    req = sum((lane >= ctx * i).astype(jnp.int32) for i in range(1, dec))
    pos = lane - ctx * req
    length = dlen[0]
    for i in range(1, dec):
        length = jnp.where(req == i, dlen[i], length)
    seen = (row8 - (8 - dec) == req) & (pos < length)
    late_row = (iota((m, 1), 0) & 7) >= 8 - dec
    for g in range(hq // per_kv):
        qg = jnp.concatenate(
            [q8[:, (g * per_kv + h) * HD : (g * per_kv + h + 1) * HD] for h in range(per_kv)], axis=0
        )
        kg = S["dec_v"][0, :, :, g * HD : (g + 1) * HD].reshape(keys, HD)
        vg = S["dec_v"][1, :, :, g * HD : (g + 1) * HD].reshape(keys, HD)
        own_k = jnp.concatenate([n8[0][:, g * HD : (g + 1) * HD]] * per_kv, axis=0)
        own_v = jnp.concatenate([n8[1][:, g * HD : (g + 1) * HD]] * per_kv, axis=0)
        s = jnp.where(seen, dot_t(qg.astype(BF16), kg) * scale, NEG)
        s_own = jnp.sum(qg * own_k, axis=1, keepdims=True) * scale
        top = jnp.maximum(jnp.max(s, axis=1, keepdims=True), s_own)
        p = jnp.where(seen, jnp.exp(s - top), 0.0)
        p_own = jnp.exp(s_own - top)
        den = jnp.sum(p, axis=1, keepdims=True) + p_own
        o = dot(p.astype(BF16), vg) + p_own.astype(BF16).astype(F32) * own_v
        S["decs"][g * 2 : (g + 1) * 2] = jnp.where(late_row, o / den, qg).astype(BF16).reshape(2, m // 2, HD)
    def d_copy(src_t, to_t):
        return remote(
            S["decs"].at[to_t], S["decr"].at[src_t],
            S["ds_sem"].at[0], S["dr_sem"].at[0], **{CHIP: to_t // 2, CORE: to_t % 2},
        )

    for o in range(n - 1, 0, -1):
        copies.start(d_copy(t, lax.rem(t + o, n)))
    S["decr"][t] = S["decs"][t]
    for o in near_first(c)[::-1] + [0]:
        to = lax.rem(y + o, c)
        for kk in ([1] if o == 0 else [0, 1]):
            late = int(turn.index((c - o) % c) >= c // 2)
            copies.start(q_copy(t, 2 * to + lax.rem(k + kk, 2), late))

    for copy in l_own:
        copy.wait()
    arrived(S["kvn"].at[k, : c - 1], S["knr_sem"].at[0])
    arrived(S["kvp"].at[k, : c - 1], S["kpr_sem"].at[0])
    copies.sent(S["kvn"].at[k, : c - 1], S["kns_sem"].at[0])
    copies.sent(S["kvp"].at[k, : c - 1], S["kps_sem"].at[0])
    copies.sent(S["qb"].at[: n - 1], S["qs_sem"].at[0])
    copies.sent(S["decs"].at[: n - 1], S["ds_sem"].at[0])
    relay = [
        copies.start(remote(S[b].at[k], S[b].at[k], S["x_s"].at[i], S["x_r"].at[i], **{CORE: other}))
        for i, b in ((1, "kvn"), (2, "kvp"))
    ]
    chip_at = [lax.rem(y + o, c) for o in turn]
    for copy in relay:
        copy.wait()
    prefix = n * pre_dev
    for i, b in ((0, "kall"), (1, "vall")):
        for cc in range(c):
            for kk in range(2):
                at = (2 * cc + kk) * pre_dev
                S[b][at : at + pre_dev, :] = S["kvp"][kk, cc, i]
            S[b][prefix + cc * 2 * r : prefix + (cc + 1) * 2 * r, :] = jnp.concatenate(
                [S["kvn"][kk, cc, i].astype(F32) for kk in range(2)], axis=0
            ).astype(BF16)
    arrived(S["decr"].at[: n - 1], S["dr_sem"].at[0])

    block_devs = 8
    block = block_devs * r
    col = iota((1, n * r), 1)
    col_dev = sum((col >= r * i).astype(jnp.int32) for i in range(1, n))
    col_in = col - r * col_dev
    key_place = jnp.where(col_in < span, col_dev * span + col_in, 1 << 20)
    l_len.wait()
    pre_seen = iota((1, prefix), 1) < S["plen_v"][...]
    row = iota((block, 1), 0)
    row_dev = sum((row >= r * i).astype(jnp.int32) for i in range(1, block_devs))
    row_in = row - r * row_dev
    blank = jnp.zeros((r - 8, HD), F32)
    att_copies = []
    for b in range(n // block_devs):
        arrived(S["qb"].at[: block_devs - b], S["qr_sem"].at[b])
        for cc in range(b * c // 2, (b + 1) * c // 2):
            pair = [2 * chip_at[cc] + i for i in range(2)]
            body = [S["qb"][device].astype(F32) for device in pair]
            for j in range(hd_dev):
                S["qh"][j * n * r + cc * 2 * r : j * n * r + (cc + 1) * 2 * r, :] = jnp.concatenate(
                    [
                        piece
                        for device, q in zip(pair, body)
                        for piece in (q[:, j * HD : (j + 1) * HD], S["decr"][device, 8 * j : 8 * j + 8].astype(F32))
                    ],
                    axis=0,
                ).astype(BF16)
        chip = sum(
            jnp.where((row_dev >> 1) == i, chip_at[b * block_devs // 2 + i], 0) for i in range(block_devs // 2)
        )
        device = 2 * chip + (row_dev & 1)
        new_seen = key_place <= device * span + row_in
        first = b * block
        for j in range(hd_dev):
            q = S["qh"][j * n * r + first : j * n * r + first + block, :]
            s1 = jnp.where(pre_seen, dot_t(q, S["kall"][:prefix, :]), NEG)
            s2 = jnp.where(new_seen, dot_t(q, S["kall"][prefix:, :]), NEG)
            top = jnp.maximum(jnp.max(s1, axis=1, keepdims=True), jnp.max(s2, axis=1, keepdims=True))
            p1 = jnp.exp((s1 - top) * scale)
            p2 = jnp.exp((s2 - top) * scale)
            den = jnp.sum(p1, axis=1, keepdims=True) + jnp.sum(p2, axis=1, keepdims=True)
            o = (dot(p1.astype(BF16), S["vall"][:prefix, :]) + dot(p2.astype(BF16), S["vall"][prefix:, :])) / den
            own = jnp.concatenate(
                [
                    piece
                    for at in chip_at[b * c // 2 : (b + 1) * c // 2]
                    for i in range(2)
                    for piece in (blank, S["decr"][2 * at + i, 8 * j : 8 * j + 8].astype(F32))
                ],
                axis=0,
            )
            S["att"][first : first + block, cols(k * jw + j * HD, HD)] = jnp.where(
                row_in < span, o, own
            ).astype(BF16)
        view = S["att"].at[first : first + block, cols(k * jw, jw)]
        att_copies.append(copies.start(remote(
            view, view, S["x_s"].at[3 + b], S["x_r"].at[3 + b], **{CORE: other},
        )))
    l_w.wait()
    wo_copy.wait()

    width, subs, wide = half // PIECES, PIECES // 2, PIECES // CHUNKS
    row_of = {o: i * 2 * r for i, o in enumerate(turn)}

    def share(o, h, sub):
        first = (h * subs + sub) * width
        return S["part"][row_of[o] : row_of[o] + 2 * r, first : first + width]

    ring = RingSum(y, c, copies, share, S["rs_out"], S["rs_in"], S["rs_s"], S["rs_r"], subs)
    for b, copy in enumerate(att_copies):
        copy.wait()
        these = slice(b * block, (b + 1) * block)
        for sub in range(0, subs, wide):
            for h in range(2):
                first = (h * subs + sub) * width
                S["part"][these, first : first + wide * width] = dot(
                    S["att"][these, :], S["wo"][:, first : first + wide * width]
                )
                if b == 0:
                    for s in range(sub, sub + wide):
                        ring.first(1, s, h)
                        ring.first(0, s, 1 - h)
    for index in sorted(range(2, len(ring.order)), key=lambda i: -(2 * ring.order[i][1] + (not ring.order[i][0]))):
        for sub in range(subs):
            ring.send(index, sub)
    sums = [ring.totals(sub) for sub in range(subs)]
    return [sums[sub][h] for h in range(2) for sub in range(subs)]


def entry_barrier(y, k, chips, x=None, groups=0):
    def greet():
        barrier = pltpu.get_barrier_semaphore()
        for o in range(chips):
            for kk in ([1] if o == 0 else [0, 1]):
                pl.semaphore_signal(
                    barrier, inc=1,
                    device_id={CHIP: lax.rem(y + o, chips), CORE: lax.rem(k + kk, 2)},
                    device_id_type=MESH,
                )
        for o in range(1, groups):
            pl.semaphore_signal(
                barrier, inc=1, device_id={EXP: lax.rem(x + o, groups)}, device_id_type=MESH
            )
        pl.semaphore_wait(barrier, 2 * chips - 1 + max(groups - 1, 0))

    return greet


def moe_scratch(d):
    r, c, groups, model, ff = d["rows"], d["chips"], d["groups"], d["model"], d["ff_dev"]
    half, slots, take = model // 2, 16, 2 * CAP
    far, nq, msgs = c // 2, CHUNKS, len(ring_order(c))
    v, dma = pltpu.VMEM, pltpu.SemaphoreType.DMA
    return dict(
        ids_v=v((2, r), jnp.int32),
        gain_v=v((1, model), F32),
        router_v=v((d["experts"], model), BF16),
        ids_b=v((2, r, 128), jnp.int32),
        hin=v((2, r, half), BF16),
        res=v((2 * r, half), F32),
        stat=v((2, 2 * r, 128), F32),
        pick=v((2, 2 * r, 128), F32),
        normed=v((2 * r, half), BF16),
        wg=v((model, ff), BF16),
        wu=v((model, ff), BF16),
        wd=v((2, ff, half), BF16),
        xs=v((groups, slots, half), BF16),
        xr=v((groups, slots, half), BF16),
        xg=v((2, c, groups * take, half), BF16),
        hid=v((2, c * groups * take, ff), BF16),
        part2=v((c * groups * take, half), F32),
        gu=v((2, 2 * groups * take, ff), F32),
        rs2_out=v((2, msgs, nq // 2, groups * take, half // nq), BF16),
        rs2_in=v((2, msgs, nq // 2, groups * take, half // nq), BF16),
        ys=v((groups, slots, half), BF16),
        yr=v((groups, slots, half), BF16),
        fin=v((2, 2 * r, half), F32),
        m_l=dma((8,)),
        m_s=dma((5,)),
        m_r=dma((5,)),
        xs_s=dma((1,)),
        xs_r=dma((nq,)),
        ag_s=dma((1,)),
        ag_r=dma((far, nq)),
        pc_s=dma((1,)),
        pc_r=dma((far + 1,)),
        h_s=dma((1,)),
        h_r=dma((far + 1,)),
        rs2_s=dma((1,)),
        rs2_r=dma((msgs, nq // 2)),
        ys_s=dma((1,)),
        ys_r=dma((nq,)),
        f_s=dma((1,)),
        f_r=dma((1,)),
    )


class Experts:
    def __init__(self, d, S, x, y, k, copies, hidden_hbm, ids, gain, router_t, wg_hbm, wu_hbm, wd_hbm, out):
        self.d, self.S, self.x, self.y, self.k, self.copies = d, S, x, y, k, copies
        self.hidden_hbm, self.ids, self.gain, self.router_t = hidden_hbm, ids, gain, router_t
        self.wg_hbm, self.wu_hbm, self.wd_hbm, self.out = wg_hbm, wu_hbm, wd_hbm, out

    def early(self):
        self.ids_load = pltpu.make_async_copy(self.ids, self.S["ids_v"], self.S["m_l"].at[4])
        self.ids_load.start()

    def load(self):
        S, k, d = self.S, self.k, self.d
        half, other = d["model"] // 2, 1 - self.k
        r = d["rows"]
        self.ids_load.wait()
        one = (iota((r, r), 0) == iota((r, r), 1)).astype(BF16)
        ids = dot_t(one, S["ids_v"][...].astype(F32).astype(BF16)).astype(jnp.int32)
        lane = iota((r, 128), 1)
        S["ids_b"][k] = jnp.where(lane < 64, ids[:, 0:1], ids[:, 1:2])

        def exchange(src, dst, i):
            return self.copies.start(remote(src, dst, S["m_s"].at[i], S["m_r"].at[i], **{CORE: other}))

        self.ids_copy = exchange(S["ids_b"].at[k], S["ids_b"].at[k], 0)
        self.hin_copy = exchange(self.hidden_hbm.at[:, cols(other * half, half)], S["hin"].at[k], 1)
        self.wd_copy = exchange(self.wd_hbm.at[0, :, cols(other * half, half)], S["wd"].at[k], 2)
        self.exchange = exchange
        self.loads = []
        for i, (src, dst) in enumerate((
            (self.hidden_hbm.at[:, cols(k * half, half)], S["hin"].at[k]),
            (self.wg_hbm.at[0], S["wg"]),
            (self.wu_hbm.at[0], S["wu"]),
            (self.wd_hbm.at[0, :, cols(k * half, half)], S["wd"].at[k]),
            (self.gain, S["gain_v"]),
            (self.router_t, S["router_v"]),
        )):
            copy = pltpu.make_async_copy(src, dst, S["m_l"].at[i if i < 4 else i + 1])
            copy.start()
            self.loads.append(copy)

    def away(self, o):
        return min(o, self.d["chips"] - o)

    def chip(self, o):
        return self.y if o == 0 else lax.rem(self.y + o, self.d["chips"])

    def route(self):
        S, d = self.S, self.d
        r = d["rows"]
        self.ids_copy.wait()
        ids = S["ids_b"][...].reshape(2 * r, 128)
        lane, row = iota((2 * r, 128), 1), iota((2 * r, 128), 0)
        expert, slot = lane >> 4, lane & 15
        self.first = ids[:, 0:1] == expert
        hot = self.first | (ids[:, 64:65] == expert)
        a, b = iota((2 * r, 2 * r), 0), iota((2 * r, 2 * r), 1)
        below = ((b < a) & ((a < r) == (b < r))).astype(BF16)
        rank = dot(below, hot.astype(BF16)).astype(jnp.int32) + jnp.where(row < r, 0, CAP)
        self.placed = hot & (rank == slot)
        one = (iota((128, 128), 0) == iota((128, 128), 1)).astype(BF16)
        self.to_slots = dot_t(one, self.placed.astype(BF16)).astype(BF16)
        self.ids2 = ids
        self.hin_copy.wait()
        for i in (0, 4, 5):
            self.loads[i].wait()

    def ffn_gate_up(self, offs, mine):
        S, d = self.S, self.d
        half, n, width = d["model"] // 2, d["groups"] * 2 * CAP, d["ff_dev"] // 2
        h = self.k if mine else 1 - self.k
        lhs = jnp.concatenate([S["xg"][h, self.chip(o)] for o in offs], axis=0)
        some = slice(0, len(offs) * n)
        for tile in range(2):
            at = slice(tile * width, (tile + 1) * width)
            gate = dot(lhs, S["wg"][rows(h * half, half, 16), at])
            up = dot(lhs, S["wu"][rows(h * half, half, 16), at])
            if mine:
                S["gu"][0, some, at] = gate
                S["gu"][1, some, at] = up
                continue
            gate = gate + S["gu"][0, some, at]
            up = up + S["gu"][1, some, at]
            act = (gate / (1.0 + jnp.exp(-gate)) * up).astype(BF16)
            for i, o in enumerate(offs):
                S["hid"][self.k, rows(self.chip(o) * n, n, 16), at] = act[i * n : (i + 1) * n]

    def hid_copy(self, o):
        n = self.d["groups"] * 2 * CAP
        view = self.S["hid"].at[self.k, rows(self.chip(o) * n, n, 16)]
        return remote(view, view, self.S["h_s"].at[0], self.S["h_r"].at[self.away(o)], **{CORE: 1 - self.k})

    def ffn_down(self, offs, mine, after=None):
        S, d = self.S, self.d
        half, n = d["model"] // 2, d["groups"] * 2 * CAP
        h = self.k if mine else 1 - self.k
        lhs = jnp.concatenate([S["hid"][h, rows(self.chip(o) * n, n, 16), :] for o in offs], axis=0)

        def tile(at):
            value = dot(lhs, S["wd"][h, :, at])
            for j, o in enumerate(offs):
                place = rows(self.chip(o) * n, n, 16)
                more = value[j * n : (j + 1) * n]
                S["part2"][place, at] = more if mine else S["part2"][place, at] + more

        def step(i, carry):
            tile(cols(i * 256, 256))
            return carry

        width, subs = half // CHUNKS, CHUNKS // 2
        if after is None:
            lax.fori_loop(0, half // 256, step, 0)
        else:
            for sub in range(subs):
                for half_of in range(2):
                    first = (half_of * subs + sub) * width
                    tile(slice(first, first + width))
                    after(half_of, sub)

    def ffn(self, offs, stage, after=None):
        if stage == 0:
            self.ffn_gate_up(offs, True)
        elif stage == 1:
            arrived(self.S["xg"].at[0, : len(offs)], self.S["pc_r"].at[self.away(offs[0])])
            self.ffn_gate_up(offs, False)
            for o in offs:
                self.copies.start(self.hid_copy(o))
        elif stage == 3:
            self.ffn_down(offs, True)
            n = self.d["groups"] * 2 * CAP
            arrived(self.S["hid"].at[0, : len(offs) * n], self.S["h_r"].at[self.away(offs[0])])
            self.ffn_down(offs, False, after)

    def chunk(self, q):
        w = self.d["model"] // 2 // CHUNKS
        return slice(q * w, (q + 1) * w)

    def partner_copy(self, o, q):
        S = self.S
        view = S["xg"].at[self.k, self.chip(o), :, self.chunk(q)]
        return remote(view, view, S["pc_s"].at[0], S["pc_r"].at[self.away(o)], **{CORE: 1 - self.k})

    def hops(self, way, q):
        far = self.d["chips"] // 2
        return far if ((q // (CHUNKS // 2)) ^ way) == 0 else far - 1

    def gather_copy(self, way, hop, q):
        S, c = self.S, self.d["chips"]
        back = hop - 1
        src = self.chip((c - back) % c if way == 0 else back % c)
        to = self.chip(1 if way == 0 else c - 1)
        view = S["xg"].at[self.k, src, :, self.chunk(q)]
        return remote(view, view, S["ag_s"].at[0], S["ag_r"].at[hop - 1, q], **{CHIP: to})

    def swap(self, send, recv, s_sem, r_sem, src_x, to_x, q):
        S = self.S
        return remote(
            S[send].at[to_x, :, self.chunk(q)], S[recv].at[src_x, :, self.chunk(q)],
            S[s_sem].at[0], S[r_sem].at[q], **{EXP: to_x},
        )

    def run(self, totals):
        S, d, x, y, k, copies = self.S, self.d, self.x, self.y, self.k, self.copies
        r, c, groups, model = d["rows"], d["chips"], d["groups"], d["model"]
        half, far, n = model // 2, c // 2, groups * 2 * CAP
        w = half // CHUNKS
        res = S["hin"][...].astype(F32).reshape(2 * r, half) + jnp.concatenate(totals, axis=1)
        S["res"][...] = res
        S["stat"][k] = jnp.broadcast_to(jnp.sum(res * res, axis=1, keepdims=True), (2 * r, 128))
        stat_copy = self.exchange(S["stat"].at[k], S["stat"].at[k], 3)
        stat_copy.wait()
        mean = (S["stat"][0][:, 0:1] + S["stat"][1][:, 0:1]) / model
        gain = S["gain_v"][:, cols(k * half, half)]
        S["normed"][...] = (S["res"][...] * lax.rsqrt(mean + 1e-05) * gain).astype(BF16)

        near = [lax.rem(x + o, groups) for o in near_first(groups)[::-1]]
        for q in range(CHUNKS):
            at = self.chunk(q)
            S["xs"][:, :, at] = dot(self.to_slots, S["normed"][:, at]).astype(BF16).reshape(groups, 16, w)
            for to in near:
                copies.start(self.swap("xs", "xr", "xs_s", "xs_r", x, to, q))
        S["xr"][x] = S["xs"][x]
        normed = S["normed"][...]
        logits = dot_t(normed, S["router_v"][:, cols(k * half, half)])
        e8 = iota(logits.shape, 1)
        ids = self.ids2
        lane = iota((2 * r, 128), 1)
        chosen = [
            jnp.sum(jnp.where(e8 == ids[:, 64 * i : 64 * i + 1], logits, 0.0), axis=1, keepdims=True)
            for i in range(2)
        ]
        S["pick"][k] = jnp.where(lane < 64, chosen[0], chosen[1])
        pick_copy = self.exchange(S["pick"].at[k], S["pick"].at[k], 4)

        ja, jb = iota((n, 128), 1), iota((n, 128), 0)
        dense = (((ja >> 4) * (2 * CAP) + (ja & 15) == jb) & ((ja & 15) < 2 * CAP)).astype(BF16)
        def pass_on(hop, q):
            ways = [way for way in range(2) if hop <= self.hops(way, q)]
            arrived(S["xg"].at[k, : len(ways), :, self.chunk(q)], S["ag_r"].at[hop - 1, q])
            for way in ways:
                if hop < self.hops(way, q):
                    copies.start(self.gather_copy(way, hop + 1, q))
            for way in ways:
                copies.start(self.partner_copy(c - hop if way == 0 else hop, q))

        ahead = 2
        for q in range(CHUNKS):
            at = self.chunk(q)
            arrived(S["xr"].at[: groups - 1, :, at], S["xs_r"].at[q])
            S["xg"][k, y, :, at] = dot(dense, S["xr"][:, :, at].reshape(groups * 16, w)).astype(BF16)
            for way in range(2):
                copies.start(self.gather_copy(way, 1, q))
            copies.start(self.partner_copy(0, q))
            if q >= ahead:
                pass_on(1, q - ahead)
        for load in self.loads[1:4]:
            load.wait()
        self.wd_copy.wait()

        quarter, subs = half // CHUNKS, CHUNKS // 2

        def share(o, h, sub):
            first = (h * subs + sub) * quarter
            return S["part2"][rows(self.chip(o) * n, n, 16), first : first + quarter]

        ring = RingSum(y, c, copies, share, S["rs2_out"], S["rs2_in"], S["rs2_s"], S["rs2_r"], subs)
        blocks = [[0]] + [[c - s, s] for s in range(1, far)] + [[far]]
        for hop in range(1, far):
            for q in range(CHUNKS):
                if hop > 1 or q >= CHUNKS - ahead:
                    pass_on(hop, q)
                self.ffn(blocks[hop - 1], q)
        self.ffn(blocks[far - 1], 0)
        for q in range(CHUNKS // 2):
            pass_on(far, q)
        self.ffn(blocks[far - 1], 1)
        for q in range(CHUNKS // 2, CHUNKS):
            pass_on(far, q)
        self.ffn(blocks[far - 1], 3, lambda h, sub: ring.first(0, sub, 1 - h))
        for stage in range(CHUNKS):
            self.ffn(blocks[far], stage, lambda h, sub: ring.first(1, sub, h))

        pick_copy.wait()
        l0 = S["pick"][0][:, 0:1] + S["pick"][1][:, 0:1]
        l1 = S["pick"][0][:, 64:65] + S["pick"][1][:, 64:65]
        top = jnp.maximum(l0, l1)
        e0, e1 = jnp.exp(l0 - top), jnp.exp(l1 - top)
        weight = jnp.where(self.placed, jnp.where(self.first, e0, e1) / (e0 + e1), 0.0)
        w_hi = weight.astype(BF16)
        w_lo = (weight - w_hi.astype(F32)).astype(BF16)
        ja, jb = iota((128, n), 0), iota((128, n), 1)
        spread = (((ja >> 4) * (2 * CAP) + (ja & 15) == jb) & ((ja & 15) < 2 * CAP)).astype(BF16)
        for kind, index, sub in ring_schedule(c, subs, RING_WIRE, RING_TURN, RING_SPREAD, RING_LATE):
            if kind == 0:
                ring.send(index, sub)
                continue
            for h, value in enumerate(ring.totals(sub)):
                q = h * subs + sub
                at = self.chunk(q)
                S["ys"][:, :, at] = dot(spread, value.astype(BF16)).astype(BF16).reshape(groups, 16, w)
                for to in near:
                    copies.start(self.swap("ys", "yr", "ys_s", "ys_r", x, to, q))
        S["yr"][x] = S["ys"][x]

        def back(q):
            view = S["fin"].at[k, rows((1 - k) * r, r, 8), self.chunk(q)]
            return remote(view, view, S["f_s"].at[0], S["f_r"].at[0], **{CORE: 1 - k})

        for q in [h * subs + sub for sub in range(subs) for h in range(2)]:
            at = self.chunk(q)
            arrived(S["yr"].at[: groups - 1, :, at], S["ys_r"].at[q])
            got = S["yr"][:, :, at].reshape(groups * 16, w)
            S["fin"][k, :, at] = S["res"][:, at] + dot(w_hi, got) + dot(w_lo, got)
            copies.start(back(q))
        arrived(S["fin"].at[1 - k, rows(k * r, r, 8), :], S["f_r"].at[0])
        for h in range(2):
            self.out[:, h * half : (h + 1) * half] = S["fin"][h, rows(k * r, r, 8), :]
        copies.sent(S["xs"].at[: groups - 1], S["xs_s"].at[0])
        copies.sent(S["ys"].at[: groups - 1], S["ys_s"].at[0])
        copies.sent(S["xg"].at[0, : c - 1], S["ag_s"].at[0])
        copies.sent(S["xg"].at[0], S["pc_s"].at[0])
        copies.sent(S["hid"].at[0], S["h_s"].at[0])
        copies.sent(S["fin"].at[k, rows((1 - k) * r, r, 8), :], S["f_s"].at[0])


def on_device(
    hidden_in,
    queries,
    new_kv,
    prefix_kv,
    decode_kv,
    prefix_len,
    decode_len,
    out_proj,
    norm_gain,
    router_w,
    expert_ids,
    w_gate,
    w_up,
    w_down,
):
    chips, hq, kvw = lax.axis_size(CHIP), queries.shape[1] // HD, new_kv.shape[2]
    d = dict(
        rows=hidden_in.shape[0], model=hidden_in.shape[1], kvw=kvw, chips=chips, heads_q=hq,
        per_kv=hq // (kvw // HD), heads_dev=hq // (2 * chips), pre_dev=prefix_kv.shape[2],
        dec=decode_len.shape[0], ctx=decode_kv.shape[2], groups=lax.axis_size(EXP), ff_dev=w_gate.shape[2],
        experts=router_w.shape[1],
    )
    scratch = {**k1_scratch(d), **moe_scratch(d)}
    names = list(scratch)

    def kernel(q, nkv, pre, dec, plen, dlen, wo, hid, ids, gain, router, wg, wu, wd, out, *rest):
        S = dict(zip(names, rest))
        x, y, k = lax.axis_index(EXP), lax.axis_index(CHIP), lax.axis_index(CORE)
        copies = Copies()
        experts = Experts(d, S, x, y, k, copies, hid, ids, gain, router, wg, wu, wd, out)
        experts.early()
        totals = attend_and_project(
            d, S, y, k, copies, q, nkv, pre, dec, plen, dlen, wo,
            entry_barrier(y, k, chips, x, d["groups"]), experts.load,
        )
        experts.route()
        experts.run(totals)
        copies.drain()

    anys = pl.BlockSpec(memory_space=pl.ANY)
    smem = pl.BlockSpec(memory_space=pltpu.SMEM)
    vmem = pl.BlockSpec(memory_space=pltpu.VMEM)
    return pl.pallas_call(
        kernel,
        out_shape=jax.ShapeDtypeStruct(hidden_in.shape, F32),
        in_specs=[anys] * 5 + [smem] + [anys] * 8,
        out_specs=vmem,
        scratch_shapes=list(scratch.values()),
        compiler_params=pltpu.CompilerParams(collective_id=0, has_side_effects=True),
        name="layer",
    )(
        queries, new_kv, prefix_kv, decode_kv, prefix_len.reshape(1, 1), decode_len, out_proj, hidden_in, expert_ids.T,
        norm_gain.reshape(1, -1), router_w.T, w_gate, w_up, w_down,
    ).astype(BF16)


def solution(mesh):
    split = Mesh(
        mesh.devices.reshape(mesh.shape["rep"], mesh.shape["exp"], mesh.shape["ten"] // 2, 2),
        ("rep", "exp", "ten_0", "ten_1"),
    )
    return jax.shard_map(
        on_device,
        mesh=split,
        in_specs=(
            P(REP_EXP_TEN, None),
            P(REP_EXP_TEN, None),
            P(None, REP_EXP_TEN, None),
            P(None, ("rep", "exp"), TEN, None),
            P(None, REP_EXP_TEN, None, None),
            P(("rep", "exp")),
            P(REP_EXP_TEN),
            P(TEN, None),
            P(),
            P(),
            P(REP_EXP_TEN, None),
            P("exp", None, TEN),
            P("exp", None, TEN),
            P("exp", TEN, None),
        ),
        out_specs=P(REP_EXP_TEN, None),
        check_vma=False,
    )
```

```python
import jax
import jax.numpy as jnp
from jax import lax
from jax.experimental import pallas as pl
from jax.experimental.pallas import tpu as pltpu
from jax.sharding import Mesh
from jax.sharding import PartitionSpec as P

MESH = pl.DeviceIdType.MESH
HD = 128
CAP = 7
F32 = jnp.float32
BF16 = jnp.bfloat16
NEG = -1e30
CHUNKS = 6
PIECES = 12
RING_WIRE, RING_TURN, RING_SPREAD, RING_LATE = 1.25, 3.2, 5.0, 2.0
EXP, CHIP, CORE = "exp", "ten_0", "ten_1"
TEN = (CHIP, CORE)
REP_EXP_TEN = ("rep", EXP, CHIP, CORE)


def iota(shape, dim):
    return lax.broadcasted_iota(jnp.int32, shape, dim)


def cols(start, size):
    return pl.ds(pl.multiple_of(start, 128), size)


def rows(start, size, align):
    return pl.ds(pl.multiple_of(start, align), size)


def dot(a, b):
    return jnp.dot(a, b, preferred_element_type=F32)


def dot_t(a, b):
    return lax.dot_general(a, b, (((1,), (1,)), ((), ())), preferred_element_type=F32)


def ring_order(chips):
    far = chips // 2
    order = []
    for hop in range(far - 1, 0, -1):
        order += [(False, hop), (True, hop + 1)]
    return order + [(True, 1)]


def ring_schedule(chips, subs, wire, turn, spread, late):
    order = ring_order(chips)
    place = {m: i for i, m in enumerate(order)}
    arrive, clock = {}, 0.0
    for index in (0, 1):
        clock = max(clock, 4.0 * index)
        for sub in range(subs):
            clock += wire
            arrive[index, sub] = clock + turn
    waiting = [(index, sub) for index in range(2, len(order)) for sub in range(subs)]
    steps = []
    while waiting:
        ready = {
            (index, sub): arrive.get((place[order[index][0], order[index][1] + 1], sub), 1e9)
            for index, sub in waiting
        }
        clock = max(clock, min(ready.values()))
        due = {m: spread * m[1] - order[m[0]][1] * (wire + turn) for m in waiting if ready[m] <= clock}
        pick = min(due, key=lambda m: (due[m], m))
        waiting.remove(pick)
        steps.append((clock, 0) + pick)
        clock += wire
        arrive[pick] = clock + turn
    last = [place[True, 1], place[False, 1]]
    for sub in range(subs):
        steps.append((max(arrive[i, sub] for i in last) + late, 1, 0, sub))
    return [step[1:] for step in sorted(steps)]


def near_first(n):
    return [(o + 1) // 2 if o % 2 else n - o // 2 for o in range(1, n)]


def ring_turns(chips):
    far = chips // 2
    return [far] + [o for d in range(far - 1, 0, -1) for o in (d, chips - d)] + [0]


class Copies:
    def __init__(self):
        self.kinds = []

    def start(self, copy):
        copy.start()
        return copy

    def sent(self, whole, sem):
        self.kinds.append((whole, sem))

    def drain(self):
        for whole, sem in self.kinds:
            arrived(whole, sem)


def arrived(whole, sem):
    pltpu.make_async_copy(whole, whole, sem).wait()


def remote(src, dst, send_sem, recv_sem, **device):
    return pltpu.make_async_remote_copy(
        src_ref=src, dst_ref=dst, send_sem=send_sem, recv_sem=recv_sem,
        device_id=device, device_id_type=MESH,
    )


class RingSum:
    def __init__(self, y, chips, copies, part, out, into, s_sem, r_sem, subs):
        self.y, self.chips, self.copies, self.part = y, chips, copies, part
        self.out, self.into, self.s_sem, self.r_sem, self.subs = out, into, s_sem, r_sem, subs
        self.order = ring_order(chips)
        self.place = {m: i for i, m in enumerate(self.order)}
        copies.sent(out, s_sem.at[0])

    def first(self, index, sub, way, before=None):
        is_long, hop = self.order[index]
        value = self.part(hop if way == 0 else self.chips - hop, (0 if is_long else 1) ^ way, sub)
        if before is not None:
            value = value + self.into[way, before, sub].astype(F32)
        self.out[way, index, sub] = value.astype(BF16)
        to = lax.rem(self.y + (1 if way == 0 else self.chips - 1), self.chips)
        self.copies.start(remote(
            self.out.at[way, index, sub], self.into.at[way, index, sub],
            self.s_sem.at[0], self.r_sem.at[index, sub], **{CHIP: to},
        ))

    def wait(self, index, sub):
        arrived(self.into.at[:, index, sub], self.r_sem.at[index, sub])

    def send(self, index, sub):
        is_long, hop = self.order[index]
        before = self.place[is_long, hop + 1]
        self.wait(before, sub)
        for way in range(2):
            self.first(index, sub, way, before)

    def totals(self, sub):
        last = [self.place[True, 1], self.place[False, 1]]
        for index in last:
            self.wait(index, sub)
        return [
            self.part(0, half, sub)
            + self.into[0, last[half], sub].astype(F32)
            + self.into[1, last[1 - half], sub].astype(F32)
            for half in range(2)
        ]


def k1_scratch(d):
    r, c, n = d["rows"], d["chips"], 2 * d["chips"]
    jw = d["heads_dev"] * HD
    half = d["model"] // 2
    msgs = len(ring_order(c))
    v, dma = pltpu.VMEM, pltpu.SemaphoreType.DMA
    return dict(
        q_v=v((r, d["heads_q"] * HD), BF16),
        nkv_v=v((2, r, d["kvw"]), BF16),
        pre_v=v((2, d["pre_dev"], d["kvw"]), BF16),
        dec_v=v((2, d["dec"], d["ctx"], d["kvw"]), BF16),
        qb=v((n, r - 8, jw), BF16),
        plen_v=v((1, 1), jnp.int32),
        kvn=v((2, c, 2, r, HD), BF16),
        kvp=v((2, c, 2, d["pre_dev"], HD), BF16),
        decs=v((n, 8 * d["heads_dev"], HD), BF16),
        decr=v((n, 8 * d["heads_dev"], HD), BF16),
        qh=v((d["heads_dev"] * n * r, HD), BF16),
        kall=v((n * (d["pre_dev"] + r), HD), BF16),
        vall=v((n * (d["pre_dev"] + r), HD), BF16),
        att=v((n * r, 2 * jw), BF16),
        wo=v((2 * jw, half), BF16),
        part=v((n * r, half), F32),
        rs_out=v((2, msgs, PIECES // 2, 2 * r, half // PIECES), BF16),
        rs_in=v((2, msgs, PIECES // 2, 2 * r, half // PIECES), BF16),
        l_sem=dma((9,)),
        qs_sem=dma((1,)),
        qr_sem=dma((2,)),
        kns_sem=dma((1,)),
        knr_sem=dma((1,)),
        kps_sem=dma((1,)),
        kpr_sem=dma((1,)),
        x_s=dma((5,)),
        x_r=dma((5,)),
        ds_sem=dma((1,)),
        dr_sem=dma((1,)),
        rs_s=dma((1,)),
        rs_r=dma((msgs, PIECES // 2)),
    )


def attend_and_project(d, S, y, k, copies, q_hbm, nkv_hbm, pre_hbm, dec_hbm, plen, dlen, wo_hbm, barrier, then):
    r, c, n, dec, span = d["rows"], d["chips"], 2 * d["chips"], d["dec"], d["rows"] - d["dec"]
    hq, per_kv, hd_dev, ctx, pre_dev = d["heads_q"], d["per_kv"], d["heads_dev"], d["ctx"], d["pre_dev"]
    jw, half = hd_dev * HD, d["model"] // 2
    t = 2 * y + k
    other = 1 - k
    scale = HD ** -0.5
    l_sem = S["l_sem"]

    def local(src, dst, i):
        copy = pltpu.make_async_copy(src, dst, l_sem.at[i])
        copy.start()
        return copy

    kv_cols = cols(y * HD, HD)
    turn = ring_turns(c)
    l_n = local(nkv_hbm, S["nkv_v"], 0)
    l_p = local(pre_hbm.at[:, 0], S["pre_v"], 1)
    l_q = local(q_hbm, S["q_v"], 2)
    l_own = [
        local(nkv_hbm.at[:, :, kv_cols], S["kvn"].at[k, y], 3),
        local(pre_hbm.at[:, 0, :, kv_cols], S["kvp"].at[k, y], 4),
        local(q_hbm.at[: r - 8, cols(t * jw, jw)], S["qb"].at[t], 5),
    ]
    l_len = local(plen, S["plen_v"], 8)
    l_d = local(dec_hbm, S["dec_v"], 6)
    l_w = local(wo_hbm.at[:, cols(k * half, half)], S["wo"].at[rows(k * jw, jw, 16)], 7)

    barrier()

    def kn_copy(src_y, to):
        return remote(
            S["nkv_v"].at[:, :, cols(to * HD, HD)], S["kvn"].at[k, src_y],
            S["kns_sem"].at[0], S["knr_sem"].at[0], **{CHIP: to},
        )

    def kp_copy(src_y, to):
        return remote(
            S["pre_v"].at[:, :, cols(to * HD, HD)], S["kvp"].at[k, src_y],
            S["kps_sem"].at[0], S["kpr_sem"].at[0], **{CHIP: to},
        )

    def q_copy(src_t, to_t, late):
        return remote(
            S["q_v"].at[: r - 8, cols(to_t * jw, jw)], S["qb"].at[src_t],
            S["qs_sem"].at[0], S["qr_sem"].at[late], **{CHIP: to_t // 2, CORE: to_t % 2},
        )

    l_n.wait()
    l_p.wait()
    for o in near_first(c)[::-1]:
        to = lax.rem(y + o, c)
        copies.start(kn_copy(y, to))
        copies.start(kp_copy(y, to))
    wo_copy = copies.start(remote(
        wo_hbm.at[:, cols(other * half, half)], S["wo"].at[rows(k * jw, jw, 16)], S["x_s"].at[0], S["x_r"].at[0],
        **{CORE: other},
    ))
    then()

    l_q.wait()
    l_d.wait()
    q8 = S["q_v"][16:24, :].astype(F32)
    n8 = [S["nkv_v"][i, 16:24, :].astype(F32) for i in range(2)]
    m = per_kv * 8
    keys = dec * ctx
    lane = iota((m, keys), 1)
    row8 = iota((m, keys), 0) & 7
    req = sum((lane >= ctx * i).astype(jnp.int32) for i in range(1, dec))
    pos = lane - ctx * req
    length = dlen[0]
    for i in range(1, dec):
        length = jnp.where(req == i, dlen[i], length)
    seen = (row8 - (8 - dec) == req) & (pos < length)
    late_row = (iota((m, 1), 0) & 7) >= 8 - dec
    for g in range(hq // per_kv):
        qg = jnp.concatenate(
            [q8[:, (g * per_kv + h) * HD : (g * per_kv + h + 1) * HD] for h in range(per_kv)], axis=0
        )
        kg = S["dec_v"][0, :, :, g * HD : (g + 1) * HD].reshape(keys, HD)
        vg = S["dec_v"][1, :, :, g * HD : (g + 1) * HD].reshape(keys, HD)
        own_k = jnp.concatenate([n8[0][:, g * HD : (g + 1) * HD]] * per_kv, axis=0)
        own_v = jnp.concatenate([n8[1][:, g * HD : (g + 1) * HD]] * per_kv, axis=0)
        s = jnp.where(seen, dot_t(qg.astype(BF16), kg) * scale, NEG)
        s_own = jnp.sum(qg * own_k, axis=1, keepdims=True) * scale
        top = jnp.maximum(jnp.max(s, axis=1, keepdims=True), s_own)
        p = jnp.where(seen, jnp.exp(s - top), 0.0)
        p_own = jnp.exp(s_own - top)
        den = jnp.sum(p, axis=1, keepdims=True) + p_own
        o = dot(p.astype(BF16), vg) + p_own.astype(BF16).astype(F32) * own_v
        S["decs"][g * 2 : (g + 1) * 2] = jnp.where(late_row, o / den, qg).astype(BF16).reshape(2, m // 2, HD)
    def d_copy(src_t, to_t):
        return remote(
            S["decs"].at[to_t], S["decr"].at[src_t],
            S["ds_sem"].at[0], S["dr_sem"].at[0], **{CHIP: to_t // 2, CORE: to_t % 2},
        )

    for o in range(n - 1, 0, -1):
        copies.start(d_copy(t, lax.rem(t + o, n)))
    S["decr"][t] = S["decs"][t]
    for o in near_first(c)[::-1] + [0]:
        to = lax.rem(y + o, c)
        for kk in ([1] if o == 0 else [0, 1]):
            late = int(turn.index((c - o) % c) >= c // 2)
            copies.start(q_copy(t, 2 * to + lax.rem(k + kk, 2), late))

    for copy in l_own:
        copy.wait()
    arrived(S["kvn"].at[k, : c - 1], S["knr_sem"].at[0])
    arrived(S["kvp"].at[k, : c - 1], S["kpr_sem"].at[0])
    copies.sent(S["kvn"].at[k, : c - 1], S["kns_sem"].at[0])
    copies.sent(S["kvp"].at[k, : c - 1], S["kps_sem"].at[0])
    copies.sent(S["qb"].at[: n - 1], S["qs_sem"].at[0])
    copies.sent(S["decs"].at[: n - 1], S["ds_sem"].at[0])
    relay = [
        copies.start(remote(S[b].at[k], S[b].at[k], S["x_s"].at[i], S["x_r"].at[i], **{CORE: other}))
        for i, b in ((1, "kvn"), (2, "kvp"))
    ]
    chip_at = [lax.rem(y + o, c) for o in turn]
    for copy in relay:
        copy.wait()
    prefix = n * pre_dev
    for i, b in ((0, "kall"), (1, "vall")):
        for cc in range(c):
            for kk in range(2):
                at = (2 * cc + kk) * pre_dev
                S[b][at : at + pre_dev, :] = S["kvp"][kk, cc, i]
            S[b][prefix + cc * 2 * r : prefix + (cc + 1) * 2 * r, :] = jnp.concatenate(
                [S["kvn"][kk, cc, i].astype(F32) for kk in range(2)], axis=0
            ).astype(BF16)
    arrived(S["decr"].at[: n - 1], S["dr_sem"].at[0])

    block_devs = 8
    block = block_devs * r
    col = iota((1, n * r), 1)
    col_dev = sum((col >= r * i).astype(jnp.int32) for i in range(1, n))
    col_in = col - r * col_dev
    key_place = jnp.where(col_in < span, col_dev * span + col_in, 1 << 20)
    l_len.wait()
    pre_seen = iota((1, prefix), 1) < S["plen_v"][...]
    row = iota((block, 1), 0)
    row_dev = sum((row >= r * i).astype(jnp.int32) for i in range(1, block_devs))
    row_in = row - r * row_dev
    blank = jnp.zeros((r - 8, HD), F32)
    att_copies = []
    for b in range(n // block_devs):
        arrived(S["qb"].at[: block_devs - b], S["qr_sem"].at[b])
        for cc in range(b * c // 2, (b + 1) * c // 2):
            pair = [2 * chip_at[cc] + i for i in range(2)]
            body = [S["qb"][device].astype(F32) for device in pair]
            for j in range(hd_dev):
                S["qh"][j * n * r + cc * 2 * r : j * n * r + (cc + 1) * 2 * r, :] = jnp.concatenate(
                    [
                        piece
                        for device, q in zip(pair, body)
                        for piece in (q[:, j * HD : (j + 1) * HD], S["decr"][device, 8 * j : 8 * j + 8].astype(F32))
                    ],
                    axis=0,
                ).astype(BF16)
        chip = sum(
            jnp.where((row_dev >> 1) == i, chip_at[b * block_devs // 2 + i], 0) for i in range(block_devs // 2)
        )
        device = 2 * chip + (row_dev & 1)
        new_seen = key_place <= device * span + row_in
        first = b * block
        for j in range(hd_dev):
            q = S["qh"][j * n * r + first : j * n * r + first + block, :]
            s1 = jnp.where(pre_seen, dot_t(q, S["kall"][:prefix, :]), NEG)
            s2 = jnp.where(new_seen, dot_t(q, S["kall"][prefix:, :]), NEG)
            top = jnp.maximum(jnp.max(s1, axis=1, keepdims=True), jnp.max(s2, axis=1, keepdims=True))
            p1 = jnp.exp((s1 - top) * scale)
            p2 = jnp.exp((s2 - top) * scale)
            den = jnp.sum(p1, axis=1, keepdims=True) + jnp.sum(p2, axis=1, keepdims=True)
            o = (dot(p1.astype(BF16), S["vall"][:prefix, :]) + dot(p2.astype(BF16), S["vall"][prefix:, :])) / den
            own = jnp.concatenate(
                [
                    piece
                    for at in chip_at[b * c // 2 : (b + 1) * c // 2]
                    for i in range(2)
                    for piece in (blank, S["decr"][2 * at + i, 8 * j : 8 * j + 8].astype(F32))
                ],
                axis=0,
            )
            S["att"][first : first + block, cols(k * jw + j * HD, HD)] = jnp.where(
                row_in < span, o, own
            ).astype(BF16)
        view = S["att"].at[first : first + block, cols(k * jw, jw)]
        att_copies.append(copies.start(remote(
            view, view, S["x_s"].at[3 + b], S["x_r"].at[3 + b], **{CORE: other},
        )))
    l_w.wait()
    wo_copy.wait()

    width, subs, wide = half // PIECES, PIECES // 2, PIECES // CHUNKS
    row_of = {o: i * 2 * r for i, o in enumerate(turn)}

    def share(o, h, sub):
        first = (h * subs + sub) * width
        return S["part"][row_of[o] : row_of[o] + 2 * r, first : first + width]

    ring = RingSum(y, c, copies, share, S["rs_out"], S["rs_in"], S["rs_s"], S["rs_r"], subs)
    for b, copy in enumerate(att_copies):
        copy.wait()
        these = slice(b * block, (b + 1) * block)
        for sub in range(0, subs, wide):
            for h in range(2):
                first = (h * subs + sub) * width
                S["part"][these, first : first + wide * width] = dot(
                    S["att"][these, :], S["wo"][:, first : first + wide * width]
                )
                if b == 0:
                    for s in range(sub, sub + wide):
                        ring.first(1, s, h)
                        ring.first(0, s, 1 - h)
    for index in sorted(range(2, len(ring.order)), key=lambda i: -(2 * ring.order[i][1] + (not ring.order[i][0]))):
        for sub in range(subs):
            ring.send(index, sub)
    sums = [ring.totals(sub) for sub in range(subs)]
    return [sums[sub][h] for h in range(2) for sub in range(subs)]


def entry_barrier(y, k, chips, x=None, groups=0):
    def greet():
        barrier = pltpu.get_barrier_semaphore()
        for o in range(chips):
            for kk in ([1] if o == 0 else [0, 1]):
                pl.semaphore_signal(
                    barrier, inc=1,
                    device_id={CHIP: lax.rem(y + o, chips), CORE: lax.rem(k + kk, 2)},
                    device_id_type=MESH,
                )
        for o in range(1, groups):
            pl.semaphore_signal(
                barrier, inc=1, device_id={EXP: lax.rem(x + o, groups)}, device_id_type=MESH
            )
        pl.semaphore_wait(barrier, 2 * chips - 1 + max(groups - 1, 0))

    return greet


def moe_scratch(d):
    r, c, groups, model, ff = d["rows"], d["chips"], d["groups"], d["model"], d["ff_dev"]
    half, slots, take = model // 2, 16, 2 * CAP
    far, nq, msgs = c // 2, CHUNKS, len(ring_order(c))
    v, dma = pltpu.VMEM, pltpu.SemaphoreType.DMA
    return dict(
        ids_v=v((2, r), jnp.int32),
        gain_v=v((1, model), F32),
        router_v=v((d["experts"], model), BF16),
        ids_b=v((2, r, 128), jnp.int32),
        hin=v((2, r, half), BF16),
        res=v((2 * r, half), F32),
        stat=v((2, 2 * r, 128), F32),
        pick=v((2, 2 * r, 128), F32),
        normed=v((2 * r, half), BF16),
        wg=v((model, ff), BF16),
        wu=v((model, ff), BF16),
        wd=v((2, ff, half), BF16),
        xs=v((groups, slots, half), BF16),
        xr=v((groups, slots, half), BF16),
        xg=v((2, c, groups * take, half), BF16),
        hid=v((2, c * groups * take, ff), BF16),
        part2=v((c * groups * take, half), F32),
        gu=v((2, 2 * groups * take, ff), F32),
        rs2_out=v((2, msgs, nq // 2, groups * take, half // nq), BF16),
        rs2_in=v((2, msgs, nq // 2, groups * take, half // nq), BF16),
        ys=v((groups, slots, half), BF16),
        yr=v((groups, slots, half), BF16),
        fin=v((2, 2 * r, half), F32),
        m_l=dma((8,)),
        m_s=dma((5,)),
        m_r=dma((5,)),
        xs_s=dma((1,)),
        xs_r=dma((nq,)),
        ag_s=dma((1,)),
        ag_r=dma((far, nq)),
        pc_s=dma((1,)),
        pc_r=dma((far + 1,)),
        h_s=dma((1,)),
        h_r=dma((far + 1,)),
        rs2_s=dma((1,)),
        rs2_r=dma((msgs, nq // 2)),
        ys_s=dma((1,)),
        ys_r=dma((nq,)),
        f_s=dma((1,)),
        f_r=dma((1,)),
    )


class Experts:
    def __init__(self, d, S, x, y, k, copies, hidden_hbm, ids, gain, router_t, wg_hbm, wu_hbm, wd_hbm, out):
        self.d, self.S, self.x, self.y, self.k, self.copies = d, S, x, y, k, copies
        self.hidden_hbm, self.ids, self.gain, self.router_t = hidden_hbm, ids, gain, router_t
        self.wg_hbm, self.wu_hbm, self.wd_hbm, self.out = wg_hbm, wu_hbm, wd_hbm, out

    def early(self):
        self.ids_load = pltpu.make_async_copy(self.ids, self.S["ids_v"], self.S["m_l"].at[4])
        self.ids_load.start()

    def load(self):
        S, k, d = self.S, self.k, self.d
        half, other = d["model"] // 2, 1 - self.k
        r = d["rows"]
        self.ids_load.wait()
        one = (iota((r, r), 0) == iota((r, r), 1)).astype(BF16)
        ids = dot_t(one, S["ids_v"][...].astype(F32).astype(BF16)).astype(jnp.int32)
        lane = iota((r, 128), 1)
        S["ids_b"][k] = jnp.where(lane < 64, ids[:, 0:1], ids[:, 1:2])

        def exchange(src, dst, i):
            return self.copies.start(remote(src, dst, S["m_s"].at[i], S["m_r"].at[i], **{CORE: other}))

        self.ids_copy = exchange(S["ids_b"].at[k], S["ids_b"].at[k], 0)
        self.hin_copy = exchange(self.hidden_hbm.at[:, cols(other * half, half)], S["hin"].at[k], 1)
        self.wd_copy = exchange(self.wd_hbm.at[0, :, cols(other * half, half)], S["wd"].at[k], 2)
        self.exchange = exchange
        self.loads = []
        for i, (src, dst) in enumerate((
            (self.hidden_hbm.at[:, cols(k * half, half)], S["hin"].at[k]),
            (self.wg_hbm.at[0], S["wg"]),
            (self.wu_hbm.at[0], S["wu"]),
            (self.wd_hbm.at[0, :, cols(k * half, half)], S["wd"].at[k]),
            (self.gain, S["gain_v"]),
            (self.router_t, S["router_v"]),
        )):
            copy = pltpu.make_async_copy(src, dst, S["m_l"].at[i if i < 4 else i + 1])
            copy.start()
            self.loads.append(copy)

    def away(self, o):
        return min(o, self.d["chips"] - o)

    def chip(self, o):
        return self.y if o == 0 else lax.rem(self.y + o, self.d["chips"])

    def route(self):
        S, d = self.S, self.d
        r = d["rows"]
        self.ids_copy.wait()
        ids = S["ids_b"][...].reshape(2 * r, 128)
        lane, row = iota((2 * r, 128), 1), iota((2 * r, 128), 0)
        expert, slot = lane >> 4, lane & 15
        self.first = ids[:, 0:1] == expert
        hot = self.first | (ids[:, 64:65] == expert)
        a, b = iota((2 * r, 2 * r), 0), iota((2 * r, 2 * r), 1)
        below = ((b < a) & ((a < r) == (b < r))).astype(BF16)
        rank = dot(below, hot.astype(BF16)).astype(jnp.int32) + jnp.where(row < r, 0, CAP)
        self.placed = hot & (rank == slot)
        one = (iota((128, 128), 0) == iota((128, 128), 1)).astype(BF16)
        self.to_slots = dot_t(one, self.placed.astype(BF16)).astype(BF16)
        self.ids2 = ids
        self.hin_copy.wait()
        for i in (0, 4, 5):
            self.loads[i].wait()

    def ffn_gate_up(self, offs, mine):
        S, d = self.S, self.d
        half, n, width = d["model"] // 2, d["groups"] * 2 * CAP, d["ff_dev"] // 2
        h = self.k if mine else 1 - self.k
        lhs = jnp.concatenate([S["xg"][h, self.chip(o)] for o in offs], axis=0)
        some = slice(0, len(offs) * n)
        for tile in range(2):
            at = slice(tile * width, (tile + 1) * width)
            gate = dot(lhs, S["wg"][rows(h * half, half, 16), at])
            up = dot(lhs, S["wu"][rows(h * half, half, 16), at])
            if mine:
                S["gu"][0, some, at] = gate
                S["gu"][1, some, at] = up
                continue
            gate = gate + S["gu"][0, some, at]
            up = up + S["gu"][1, some, at]
            act = (gate / (1.0 + jnp.exp(-gate)) * up).astype(BF16)
            for i, o in enumerate(offs):
                S["hid"][self.k, rows(self.chip(o) * n, n, 16), at] = act[i * n : (i + 1) * n]

    def hid_copy(self, o):
        n = self.d["groups"] * 2 * CAP
        view = self.S["hid"].at[self.k, rows(self.chip(o) * n, n, 16)]
        return remote(view, view, self.S["h_s"].at[0], self.S["h_r"].at[self.away(o)], **{CORE: 1 - self.k})

    def ffn_down(self, offs, mine, after=None):
        S, d = self.S, self.d
        half, n = d["model"] // 2, d["groups"] * 2 * CAP
        h = self.k if mine else 1 - self.k
        lhs = jnp.concatenate([S["hid"][h, rows(self.chip(o) * n, n, 16), :] for o in offs], axis=0)

        def tile(at):
            value = dot(lhs, S["wd"][h, :, at])
            for j, o in enumerate(offs):
                place = rows(self.chip(o) * n, n, 16)
                more = value[j * n : (j + 1) * n]
                S["part2"][place, at] = more if mine else S["part2"][place, at] + more

        def step(i, carry):
            tile(cols(i * 256, 256))
            return carry

        width, subs = half // CHUNKS, CHUNKS // 2
        if after is None:
            lax.fori_loop(0, half // 256, step, 0)
        else:
            for sub in range(subs):
                for half_of in range(2):
                    first = (half_of * subs + sub) * width
                    tile(slice(first, first + width))
                    after(half_of, sub)

    def ffn(self, offs, stage, after=None):
        if stage == 0:
            self.ffn_gate_up(offs, True)
        elif stage == 1:
            arrived(self.S["xg"].at[0, : len(offs)], self.S["pc_r"].at[self.away(offs[0])])
            self.ffn_gate_up(offs, False)
            for o in offs:
                self.copies.start(self.hid_copy(o))
        elif stage == 3:
            self.ffn_down(offs, True)
            n = self.d["groups"] * 2 * CAP
            arrived(self.S["hid"].at[0, : len(offs) * n], self.S["h_r"].at[self.away(offs[0])])
            self.ffn_down(offs, False, after)

    def chunk(self, q):
        w = self.d["model"] // 2 // CHUNKS
        return slice(q * w, (q + 1) * w)

    def partner_copy(self, o, q):
        S = self.S
        view = S["xg"].at[self.k, self.chip(o), :, self.chunk(q)]
        return remote(view, view, S["pc_s"].at[0], S["pc_r"].at[self.away(o)], **{CORE: 1 - self.k})

    def hops(self, way, q):
        far = self.d["chips"] // 2
        return far if ((q // (CHUNKS // 2)) ^ way) == 0 else far - 1

    def gather_copy(self, way, hop, q):
        S, c = self.S, self.d["chips"]
        back = hop - 1
        src = self.chip((c - back) % c if way == 0 else back % c)
        to = self.chip(1 if way == 0 else c - 1)
        view = S["xg"].at[self.k, src, :, self.chunk(q)]
        return remote(view, view, S["ag_s"].at[0], S["ag_r"].at[hop - 1, q], **{CHIP: to})

    def swap(self, send, recv, s_sem, r_sem, src_x, to_x, q):
        S = self.S
        return remote(
            S[send].at[to_x, :, self.chunk(q)], S[recv].at[src_x, :, self.chunk(q)],
            S[s_sem].at[0], S[r_sem].at[q], **{EXP: to_x},
        )

    def run(self, totals):
        S, d, x, y, k, copies = self.S, self.d, self.x, self.y, self.k, self.copies
        r, c, groups, model = d["rows"], d["chips"], d["groups"], d["model"]
        half, far, n = model // 2, c // 2, groups * 2 * CAP
        w = half // CHUNKS
        res = S["hin"][...].astype(F32).reshape(2 * r, half) + jnp.concatenate(totals, axis=1)
        S["res"][...] = res
        S["stat"][k] = jnp.broadcast_to(jnp.sum(res * res, axis=1, keepdims=True), (2 * r, 128))
        stat_copy = self.exchange(S["stat"].at[k], S["stat"].at[k], 3)
        stat_copy.wait()
        mean = (S["stat"][0][:, 0:1] + S["stat"][1][:, 0:1]) / model
        gain = S["gain_v"][:, cols(k * half, half)]
        S["normed"][...] = (S["res"][...] * lax.rsqrt(mean + 1e-05) * gain).astype(BF16)

        near = [lax.rem(x + o, groups) for o in near_first(groups)[::-1]]
        for q in range(CHUNKS):
            at = self.chunk(q)
            S["xs"][:, :, at] = dot(self.to_slots, S["normed"][:, at]).astype(BF16).reshape(groups, 16, w)
            for to in near:
                copies.start(self.swap("xs", "xr", "xs_s", "xs_r", x, to, q))
        S["xr"][x] = S["xs"][x]
        normed = S["normed"][...]
        logits = dot_t(normed, S["router_v"][:, cols(k * half, half)])
        e8 = iota(logits.shape, 1)
        ids = self.ids2
        lane = iota((2 * r, 128), 1)
        chosen = [
            jnp.sum(jnp.where(e8 == ids[:, 64 * i : 64 * i + 1], logits, 0.0), axis=1, keepdims=True)
            for i in range(2)
        ]
        S["pick"][k] = jnp.where(lane < 64, chosen[0], chosen[1])
        pick_copy = self.exchange(S["pick"].at[k], S["pick"].at[k], 4)

        ja, jb = iota((n, 128), 1), iota((n, 128), 0)
        dense = (((ja >> 4) * (2 * CAP) + (ja & 15) == jb) & ((ja & 15) < 2 * CAP)).astype(BF16)
        def pass_on(hop, q):
            ways = [way for way in range(2) if hop <= self.hops(way, q)]
            arrived(S["xg"].at[k, : len(ways), :, self.chunk(q)], S["ag_r"].at[hop - 1, q])
            for way in ways:
                if hop < self.hops(way, q):
                    copies.start(self.gather_copy(way, hop + 1, q))
            for way in ways:
                copies.start(self.partner_copy(c - hop if way == 0 else hop, q))

        ahead = 2
        for q in range(CHUNKS):
            at = self.chunk(q)
            arrived(S["xr"].at[: groups - 1, :, at], S["xs_r"].at[q])
            S["xg"][k, y, :, at] = dot(dense, S["xr"][:, :, at].reshape(groups * 16, w)).astype(BF16)
            for way in range(2):
                copies.start(self.gather_copy(way, 1, q))
            copies.start(self.partner_copy(0, q))
            if q >= ahead:
                pass_on(1, q - ahead)
        for load in self.loads[1:4]:
            load.wait()
        self.wd_copy.wait()

        quarter, subs = half // CHUNKS, CHUNKS // 2

        def share(o, h, sub):
            first = (h * subs + sub) * quarter
            return S["part2"][rows(self.chip(o) * n, n, 16), first : first + quarter]

        ring = RingSum(y, c, copies, share, S["rs2_out"], S["rs2_in"], S["rs2_s"], S["rs2_r"], subs)
        blocks = [[0]] + [[c - s, s] for s in range(1, far)] + [[far]]
        for hop in range(1, far):
            for q in range(CHUNKS):
                if hop > 1 or q >= CHUNKS - ahead:
                    pass_on(hop, q)
                self.ffn(blocks[hop - 1], q)
        self.ffn(blocks[far - 1], 0)
        self.ffn(blocks[far - 1], 1)
        self.ffn(blocks[far - 1], 3, lambda h, sub: ring.first(0, sub, 1 - h))
        for q in range(CHUNKS):
            pass_on(far, q)
        for stage in range(CHUNKS):
            self.ffn(blocks[far], stage, lambda h, sub: ring.first(1, sub, h))

        pick_copy.wait()
        l0 = S["pick"][0][:, 0:1] + S["pick"][1][:, 0:1]
        l1 = S["pick"][0][:, 64:65] + S["pick"][1][:, 64:65]
        top = jnp.maximum(l0, l1)
        e0, e1 = jnp.exp(l0 - top), jnp.exp(l1 - top)
        weight = jnp.where(self.placed, jnp.where(self.first, e0, e1) / (e0 + e1), 0.0)
        w_hi = weight.astype(BF16)
        w_lo = (weight - w_hi.astype(F32)).astype(BF16)
        ja, jb = iota((128, n), 0), iota((128, n), 1)
        spread = (((ja >> 4) * (2 * CAP) + (ja & 15) == jb) & ((ja & 15) < 2 * CAP)).astype(BF16)
        for kind, index, sub in ring_schedule(c, subs, RING_WIRE, RING_TURN, RING_SPREAD, RING_LATE):
            if kind == 0:
                ring.send(index, sub)
                continue
            for h, value in enumerate(ring.totals(sub)):
                q = h * subs + sub
                at = self.chunk(q)
                S["ys"][:, :, at] = dot(spread, value.astype(BF16)).astype(BF16).reshape(groups, 16, w)
                for to in near:
                    copies.start(self.swap("ys", "yr", "ys_s", "ys_r", x, to, q))
        S["yr"][x] = S["ys"][x]

        def back(q):
            view = S["fin"].at[k, rows((1 - k) * r, r, 8), self.chunk(q)]
            return remote(view, view, S["f_s"].at[0], S["f_r"].at[0], **{CORE: 1 - k})

        for q in [h * subs + sub for sub in range(subs) for h in range(2)]:
            at = self.chunk(q)
            arrived(S["yr"].at[: groups - 1, :, at], S["ys_r"].at[q])
            got = S["yr"][:, :, at].reshape(groups * 16, w)
            S["fin"][k, :, at] = S["res"][:, at] + dot(w_hi, got) + dot(w_lo, got)
            copies.start(back(q))
        arrived(S["fin"].at[1 - k, rows(k * r, r, 8), :], S["f_r"].at[0])
        for h in range(2):
            self.out[:, h * half : (h + 1) * half] = S["fin"][h, rows(k * r, r, 8), :].astype(BF16)
        copies.sent(S["xs"].at[: groups - 1], S["xs_s"].at[0])
        copies.sent(S["ys"].at[: groups - 1], S["ys_s"].at[0])
        copies.sent(S["xg"].at[0, : c - 1], S["ag_s"].at[0])
        copies.sent(S["xg"].at[0], S["pc_s"].at[0])
        copies.sent(S["hid"].at[0], S["h_s"].at[0])
        copies.sent(S["fin"].at[k, rows((1 - k) * r, r, 8), :], S["f_s"].at[0])


def on_device(
    hidden_in,
    queries,
    new_kv,
    prefix_kv,
    decode_kv,
    prefix_len,
    decode_len,
    out_proj,
    norm_gain,
    router_w,
    expert_ids,
    w_gate,
    w_up,
    w_down,
):
    chips, hq, kvw = lax.axis_size(CHIP), queries.shape[1] // HD, new_kv.shape[2]
    d = dict(
        rows=hidden_in.shape[0], model=hidden_in.shape[1], kvw=kvw, chips=chips, heads_q=hq,
        per_kv=hq // (kvw // HD), heads_dev=hq // (2 * chips), pre_dev=prefix_kv.shape[2],
        dec=decode_len.shape[0], ctx=decode_kv.shape[2], groups=lax.axis_size(EXP), ff_dev=w_gate.shape[2],
        experts=router_w.shape[1],
    )
    scratch = {**k1_scratch(d), **moe_scratch(d)}
    names = list(scratch)

    def kernel(q, nkv, pre, dec, plen, dlen, wo, hid, ids, gain, router, wg, wu, wd, out, *rest):
        S = dict(zip(names, rest))
        x, y, k = lax.axis_index(EXP), lax.axis_index(CHIP), lax.axis_index(CORE)
        copies = Copies()
        experts = Experts(d, S, x, y, k, copies, hid, ids, gain, router, wg, wu, wd, out)
        experts.early()
        totals = attend_and_project(
            d, S, y, k, copies, q, nkv, pre, dec, plen, dlen, wo,
            entry_barrier(y, k, chips, x, d["groups"]), experts.load,
        )
        experts.route()
        experts.run(totals)
        copies.drain()

    anys = pl.BlockSpec(memory_space=pl.ANY)
    smem = pl.BlockSpec(memory_space=pltpu.SMEM)
    vmem = pl.BlockSpec(memory_space=pltpu.VMEM)
    return pl.pallas_call(
        kernel,
        out_shape=jax.ShapeDtypeStruct(hidden_in.shape, BF16),
        in_specs=[anys] * 5 + [smem] + [anys] * 8,
        out_specs=vmem,
        scratch_shapes=list(scratch.values()),
        compiler_params=pltpu.CompilerParams(collective_id=0, has_side_effects=True),
        name="layer",
    )(
        queries, new_kv, prefix_kv, decode_kv, prefix_len.reshape(1, 1), decode_len, out_proj, hidden_in, expert_ids.T,
        norm_gain.reshape(1, -1), router_w.T, w_gate, w_up, w_down,
    )


def solution(mesh):
    split = Mesh(
        mesh.devices.reshape(mesh.shape["rep"], mesh.shape["exp"], mesh.shape["ten"] // 2, 2),
        ("rep", "exp", "ten_0", "ten_1"),
    )
    return jax.shard_map(
        on_device,
        mesh=split,
        in_specs=(
            P(REP_EXP_TEN, None),
            P(REP_EXP_TEN, None),
            P(None, REP_EXP_TEN, None),
            P(None, ("rep", "exp"), TEN, None),
            P(None, REP_EXP_TEN, None, None),
            P(("rep", "exp")),
            P(REP_EXP_TEN),
            P(TEN, None),
            P(),
            P(),
            P(REP_EXP_TEN, None),
            P("exp", None, TEN),
            P("exp", None, TEN),
            P("exp", TEN, None),
        ),
        out_specs=P(REP_EXP_TEN, None),
        check_vma=False,
    )
```
